1024 devices in a mesh: gx: 32 (over z), gy: 4 (over y), gz: 8 (over x, core).
Axes of the slice: x: 4, y: 4, z: 32, core: 2. Of those that a mesh axis runs over, the one named last changes fastest.
Arguments:
- positions: float32 [3, 128, 16, 1024], P(None, 'gx', 'gy', 'gz'), may hold values from 0.6 to 13.9, as said below
- counts: int32 [128, 16, 16], P('gx', 'gy', 'gz'), may hold values from 24 to 64
Outputs:
- forces: float32 [3, 128, 16, 1024], P(None, 'gx', 'gy', 'gz')
- energy: float32 [128, 16, 1024], P('gx', 'gy', 'gz')
The draws below stay inside these ranges and needn't reach their ends.
Inputs may be any that keep to these rules, and one draw needn't show every extreme that they name: `positions`: each cell is a box of 2a x 2a x 4a with a = 3.615 and every atom lies inside its own cell's box; two atoms are 1.0 or more apart, and no atom is within 5.51 of an atom outside its cell's 27 neighbour cells.
All inputs are finite; a program needn't handle non-finite values.
Results may differ from the reference program's by a relative error of at most 0.0003.
Values sent between devices are 32-bit elements; how exact they have to be, the bound alone decides.
No kernel may reach another device: no remote copies, remote signals or barrier semaphores. Data moves between devices by JAX's collectives and lax.ppermute only.
A program may use at most 32 MiB of HBM per device.

```python
import jax
import jax.numpy as jnp
from jax import lax

CX = 4
SLOTS = 64
NX = 128
NY = 16
NZ = 16
N_GX = 32


lattice_const = 3.615


def site_table():
    site_index = jnp.arange(64, dtype=jnp.int32)
    basis_id = site_index % 4
    unit_id = site_index // 4
    unit_x = (unit_id % 2).astype(jnp.float32)
    unit_y = (unit_id // 2 % 2).astype(jnp.float32)
    unit_z = (unit_id // 4).astype(jnp.float32)
    half_x = jnp.where((basis_id == 2) | (basis_id == 3), 0.5, 0.0)
    half_y = jnp.where((basis_id == 1) | (basis_id == 3), 0.5, 0.0)
    half_z = jnp.where((basis_id == 1) | (basis_id == 2), 0.5, 0.0)
    return jnp.stack([unit_x + half_x + 0.25, unit_y + half_y + 0.25, unit_z + half_z + 0.25]) * lattice_const


def permute_slots(cell_key):
    return jax.random.permutation(cell_key, 64)[:SLOTS]


def draw_positions(key, part):
    cell_count = NX * NY * NZ
    cell_keys = jax.random.split(jax.random.fold_in(key, 7), cell_count)
    chosen = jax.vmap(permute_slots)(cell_keys)
    base = site_table()[:, chosen]
    noise_key = jax.random.fold_in(key, 8)
    jitter = jnp.clip(0.08 * jax.random.normal(noise_key, (3, cell_count, SLOTS), jnp.float32), -0.25, 0.25)
    placed = base + jitter
    reach = jax.random.uniform(jax.random.fold_in(key, 9), (cell_count,), jnp.float32, 1.0, 1.15)
    chosen_cells = jax.random.randint(jax.random.fold_in(key, 10), (cell_count,), 0, 2) == 1
    heading = jnp.where(base[0, :, 0] > lattice_const, -1.0, 1.0)
    zeros_row = jnp.zeros((cell_count,), jnp.float32)
    moved = placed[:, :, 0] + jnp.stack([heading * reach, zeros_row, zeros_row])
    second = jnp.where(chosen_cells[None, :], moved, placed[:, :, 1])
    placed = jnp.concatenate([placed[:, :, :1], second[:, :, None], placed[:, :, 2:]], axis=2)
    return placed.reshape(3, NX, NY, NZ * SLOTS).astype(jnp.float32)


def touch_ends(values, own_key, low, high):
    place = [jax.random.randint(jax.random.fold_in(own_key, axis), (), 0, length) for axis, length in enumerate(values.shape)]
    main_axis = values.shape.index(max(values.shape))
    neighbour = place[:main_axis] + [(place[main_axis] + 1) % values.shape[main_axis]] + place[main_axis + 1:]
    return values.at[tuple(place)].set(low).at[tuple(neighbour)].set(high)


def setup_inputs(seed: int = 0) -> dict:
    streams_of = jax.random.split(jax.random.key(seed), 3)
    positions = draw_positions(jax.random.fold_in(streams_of[2], 71), 0)
    counts = touch_ends(jax.random.randint(streams_of[1], (NX, NY, NZ), SLOTS * 3 // 8, SLOTS + 1), jax.random.fold_in(streams_of[1], 1), SLOTS * 3 // 8, SLOTS).astype(jnp.int32)
    return dict(positions=positions, counts=counts)


lattice_const = 3.615
cell_span = (2.0 * lattice_const, 2.0 * lattice_const, 4.0 * lattice_const)
cut_radius = 5.50679
cut_width = 0.50037
dens_scale = 3.80362
beta_one = 0.17394
radius_three = -2.19885
energy_one = 201.458
energy_two = 0.00659288
radius_one = 0.83591
radius_two = 4.46867
alpha_one = 2.97758
alpha_two = 1.54927
shift_delta = 0.0086225
repulsion = ((4.0, 2.24), (40.0, 1.8), (1150.0, 1.2))
embed_zero = -2.28235
embed_curve = 1.35535
lower_terms = (-1.27775, -0.86074, 1.78804, 2.97571)
upper_quartic = 0.4
upper_damping = 0.3
cell_offsets = [(first, second, third) for first in (-1, 0, 1) for second in (-1, 0, 1) for third in (-1, 0, 1)]

def tapering(radius):
    scaled = (radius - cut_radius) / cut_width
    quartic = scaled ** 4
    inside = scaled < 0.0
    taper_value = jnp.where(inside, quartic / (1.0 + quartic), 0.0)
    taper_slope = jnp.where(inside, 4.0 * scaled ** 3 / (1.0 + quartic) ** 2 / cut_width, 0.0)
    return (taper_value, taper_slope)

def gaussian_part(radius):
    return dens_scale * jnp.exp(-beta_one * (radius - radius_three) ** 2)

def radial_density(radius):
    taper_value, taper_slope = tapering(radius)
    return gaussian_part(radius) * taper_value

def morse_terms(radius, center_at, stiffness):
    decay = jnp.exp(-stiffness * (radius - center_at))
    return (decay * decay - 2.0 * decay, 2.0 * stiffness * (decay - decay * decay))

def pair_terms(radius):
    taper_value, taper_slope = tapering(radius)
    gaussian = gaussian_part(radius)
    dens_value = gaussian * taper_value
    dens_slope = gaussian * (-2.0 * beta_one * (radius - radius_three)) * taper_value + gaussian * taper_slope
    morse_first, slope_first = morse_terms(radius, radius_one, alpha_one)
    morse_second, slope_second = morse_terms(radius, radius_two, alpha_two)
    base_value = energy_one * morse_first + energy_two * morse_second + shift_delta
    base_slope = energy_one * slope_first + energy_two * slope_second
    pair_value = base_value * taper_value
    pair_slope = base_slope * taper_value + base_value * taper_slope
    for strength, reach_at in repulsion:
        closeness = jnp.maximum(reach_at - radius, 0.0)
        pair_value = pair_value - strength * closeness ** 4
        pair_slope = pair_slope + 4.0 * strength * closeness ** 3
    return (pair_value, pair_slope, dens_value, dens_slope)

def embedding(density):
    excess = density - 1.0
    below_value = embed_zero + 0.5 * embed_curve * excess ** 2 + lower_terms[0] * excess ** 3 + lower_terms[1] * excess ** 4 + lower_terms[2] * excess ** 5 + lower_terms[3] * excess ** 6
    below_slope = embed_curve * excess + 3.0 * lower_terms[0] * excess ** 2 + 4.0 * lower_terms[1] * excess ** 3 + 5.0 * lower_terms[2] * excess ** 4 + 6.0 * lower_terms[3] * excess ** 5
    numerator = embed_zero + 0.5 * embed_curve * excess ** 2 + lower_terms[0] * excess ** 3 + upper_quartic * excess ** 4
    numer_slope = embed_curve * excess + 3.0 * lower_terms[0] * excess ** 2 + 4.0 * upper_quartic * excess ** 3
    denominator = 1.0 + upper_damping * excess ** 3
    above_value = numerator / denominator
    above_slope = (numer_slope * denominator - numerator * 3.0 * upper_damping * excess ** 2) / denominator ** 2
    is_below = excess < 0.0
    return (jnp.where(is_below, below_value, above_value), jnp.where(is_below, below_slope, above_slope))

def pair_geometry(center, beside, offset):
    displace = []
    for component in range(3):
        displace.append(beside[component][..., None, :] + offset[component] * cell_span[component] - center[component][..., :, None])
    weight = center[3][..., :, None] * beside[3][..., None, :]
    if offset == (0, 0, 0):
        slot_count = center.shape[-1]
        weight = weight * (1.0 - jnp.eye(slot_count, dtype=jnp.float32))
    squared = displace[0] ** 2 + displace[1] ** 2 + displace[2] ** 2
    radius = jnp.sqrt(jnp.where(weight > 0.0, squared, 100.0))
    return (displace, weight, radius)

def shifted_cells(view_data, offset, extent):
    return view_data[:, 1 + offset[0]:1 + offset[0] + extent[0], 1 + offset[1]:1 + offset[1] + extent[1], 1 + offset[2]:1 + offset[2] + extent[2]]

def cell_density(view_data):
    extent = (view_data.shape[1] - 2, view_data.shape[2] - 2, view_data.shape[3] - 2)
    center = view_data[:, 1:-1, 1:-1, 1:-1]
    summed = jnp.zeros(center.shape[1:], jnp.float32)
    for offset in cell_offsets:
        beside = shifted_cells(view_data, offset, extent)
        displace, weight, radius = pair_geometry(center, beside, offset)
        summed = summed + lax.optimization_barrier(jnp.sum(weight * radial_density(radius), axis=-1))
    return summed

def cell_forces(view_data, slope_data):
    extent = (view_data.shape[1] - 2, view_data.shape[2] - 2, view_data.shape[3] - 2)
    center = view_data[:, 1:-1, 1:-1, 1:-1]
    slope_center = slope_data[0, 1:-1, 1:-1, 1:-1]
    force_sums = [jnp.zeros(center.shape[1:], jnp.float32) for component in range(3)]
    pair_sum = jnp.zeros(center.shape[1:], jnp.float32)
    for offset in cell_offsets:
        beside = shifted_cells(view_data, offset, extent)
        slope_beside = shifted_cells(slope_data, offset, extent)[0]
        displace, weight, radius = pair_geometry(center, beside, offset)
        pair_value, pair_slope, dens_value, dens_slope = pair_terms(radius)
        factor = weight * (pair_slope + (slope_center[..., :, None] + slope_beside[..., None, :]) * dens_slope) / radius
        force_sums = [force_sums[component] + lax.optimization_barrier(jnp.sum(factor * displace[component], axis=-1)) for component in range(3)]
        pair_sum = pair_sum + lax.optimization_barrier(jnp.sum(weight * pair_value, axis=-1))
    return (jnp.stack(force_sums), pair_sum)

def reference(positions, counts):
    occupied = (jnp.arange(SLOTS, dtype=jnp.int32)[None, None, None, :] < counts[..., None]).astype(jnp.float32)
    coords = positions.reshape(3, NX, NY, NZ, SLOTS)
    packed = jnp.concatenate([coords, occupied[None]], axis=0)
    borders = ((0, 0), (1, 1), (1, 1), (1, 1), (0, 0))
    wrapped = jnp.pad(packed, borders, mode='wrap')
    starts = (jnp.arange(N_GX, dtype=jnp.int32) * CX).astype(jnp.int32)
    index_zero = jnp.zeros((), jnp.int32)

    def density_block(first_cell):
        view_data = lax.dynamic_slice(wrapped, (index_zero, first_cell, index_zero, index_zero, index_zero), (4, CX + 2, NY + 2, NZ + 2, SLOTS))
        return cell_density(view_data)
    density = lax.map(density_block, starts).reshape(NX, NY, NZ, SLOTS)
    embed_value, embed_slope = embedding(density)
    slope = embed_slope * occupied
    slope_wrapped = jnp.pad(slope[None], borders, mode='wrap')

    def force_block(first_cell):
        view_data = lax.dynamic_slice(wrapped, (index_zero, first_cell, index_zero, index_zero, index_zero), (4, CX + 2, NY + 2, NZ + 2, SLOTS))
        slope_data = lax.dynamic_slice(slope_wrapped, (index_zero, first_cell, index_zero, index_zero, index_zero), (1, CX + 2, NY + 2, NZ + 2, SLOTS))
        return cell_forces(view_data, slope_data)
    force_blocks, pair_blocks = lax.map(force_block, starts)
    forces = jnp.moveaxis(force_blocks, 1, 0).reshape(3, NX, NY, NZ * SLOTS)
    pair_sum = pair_blocks.reshape(NX, NY, NZ, SLOTS)
    energy = (occupied * (embed_value + 0.5 * pair_sum)).reshape(NX, NY, NZ * SLOTS)
    return (forces, energy)
```

```python
import functools

import jax
import jax.numpy as jnp
import numpy as np
from jax import lax
from jax.experimental import pallas as pl
from jax.experimental.pallas import tpu as pltpu
from jax.sharding import PartitionSpec as P

SLOTS = 64
lattice_const = 3.615
SPAN_XY = 2.0 * lattice_const
SPAN_Z = 4.0 * lattice_const
cut_radius = 5.50679
cut_width = 0.50037
dens_scale = 3.80362
beta_one = 0.17394
radius_three = -2.19885
energy_one = 201.458
energy_two = 0.00659288
radius_one = 0.83591
radius_two = 4.46867
alpha_one = 2.97758
alpha_two = 1.54927
shift_delta = 0.0086225
repulsion = ((4.0, 2.24), (40.0, 1.8), (1150.0, 1.2))
embed_zero = -2.28235
embed_curve = 1.35535
lower_terms = (-1.27775, -0.86074, 1.78804, 2.97571)
upper_quartic = 0.4
upper_damping = 0.3
LOG2E = 1.4426950408889634

HB = 1.836
ZOFF = 0.228
NB = 28
CAP = 8
MAIN = NB * CAP
NSLOT = 512
NCHUNK = NSLOT // 8
FAR = 1000.0


def index_tables():
    lane = np.arange(128)
    sub = np.arange(8)[:, None]
    unit = lane // 8
    used = np.minimum(unit, 11)
    dens = []
    for row in range(7):
        for dy in (-1, 0, 1):
            col = (row + used // 6) * 8 + (used % 6 + 1 + dy)
            dens.append(np.broadcast_to(col, (8, 128)))
    back, mask = [], []
    for t in range(3):
        x, y = lane // 8 - 1, lane % 8 - 1
        ok = (lane < 64) & (x >= 2 * t) & (x < 2 * t + 2) & (y >= 0) & (y < 6)
        src = np.where(ok, ((x - 2 * t) * 6 + y) * 8, 0) + sub
        back.append(src)
        mask.append(np.broadcast_to(ok.astype(np.int32), (8, 128)))
    forc = []
    for dx in (-1, 0, 1):
        for dy in (-1, 0, 1):
            col = (unit // 4 + 2 + dx) * 8 + (unit % 4 + 2 + dy)
            forc.append(np.broadcast_to(col, (8, 128)))
    fback = np.where(lane < 16, lane * 8, 0) + sub
    tabs = np.stack(dens + back + mask + forc + [fback]).astype(np.int32)
    return tabs


T_DENS, T_BACK, T_MASK, T_FORC, T_FBACK = 0, 21, 24, 27, 36


def split3(v):
    hi = v.astype(jnp.bfloat16).astype(jnp.float32)
    rest = v - hi
    mid = rest.astype(jnp.bfloat16).astype(jnp.float32)
    return hi, mid, rest - mid


def embedding(density):
    e = density - 1.0
    e2 = e * e
    e3 = e2 * e
    l0, l1, l2, l3 = lower_terms
    low = embed_zero + e2 * (0.5 * embed_curve + e * (l0 + e * (l1 + e * (l2 + e * l3))))
    lows = e * (embed_curve + e * (3.0 * l0 + e * (4.0 * l1 + e * (5.0 * l2 + e * (6.0 * l3)))))
    num = embed_zero + e2 * (0.5 * embed_curve + e * (l0 + e * upper_quartic))
    nums = e * (embed_curve + e * (3.0 * l0 + e * (4.0 * upper_quartic)))
    below = e < 0.0
    den = jnp.where(below, 1.0, 1.0 + upper_damping * e3)
    inv = 1.0 / den
    up = num * inv
    ups = (nums * den - num * (3.0 * upper_damping) * e2) * inv * inv
    return jnp.where(below, low, up), jnp.where(below, lows, ups)


def geometry(xi, yi, zi, xj, yj, zj, mask_self):
    dx, dy, dz = xj - xi, yj - yi, zj - zi
    r2 = dx * dx + dy * dy + dz * dz
    if mask_self:
        r2 = jnp.where(r2 < 0.25, 100.0, r2)
    rinv = lax.rsqrt(r2)
    return dx, dy, dz, rinv, r2 * rinv


def rho_tile(xi, yi, zi, xj, yj, zj, mask_self):
    _, _, _, _, r = geometry(xi, yi, zi, xj, yj, zj, mask_self)
    t = jnp.minimum(r * (1.0 / cut_width) - cut_radius / cut_width, 0.0)
    t2 = t * t
    q = t2 * t2
    rs = r - radius_three
    ex = rs * (rs * (-beta_one * LOG2E)) + float(np.log2(dens_scale))
    return jnp.exp2(ex) * (q / (1.0 + q))


def force_tile(xi, yi, zi, si, xj, yj, zj, sj, mask_self):
    dx, dy, dz, rinv, r = geometry(xi, yi, zi, xj, yj, zj, mask_self)
    t = jnp.minimum(r * (1.0 / cut_width) - cut_radius / cut_width, 0.0)
    t2 = t * t
    q = t2 * t2
    inv = 1.0 / (1.0 + q)
    taper = q * inv
    tslope = (t * t2) * (inv * inv) * (4.0 / cut_width)
    rs = r - radius_three
    gr = rs * (-beta_one * LOG2E)
    g = jnp.exp2(rs * gr + float(np.log2(dens_scale)))
    dslope = g * (gr * taper * (2.0 / LOG2E) + tslope)
    u1 = jnp.exp2(r * (-alpha_one * LOG2E) + alpha_one * LOG2E * radius_one)
    u2 = jnp.exp2(r * (-alpha_two * LOG2E) + alpha_two * LOG2E * radius_two)
    y1 = u1 * (u1 - 1.0)
    y2 = u2 * (u2 - 1.0)
    base = (y1 - u1) * energy_one + ((y2 - u2) * energy_two + shift_delta)
    bslope = y1 * (-2.0 * alpha_one * energy_one) + y2 * (-2.0 * alpha_two * energy_two)
    pval = base * taper
    pslope = bslope * taper + base * tslope
    rep = None
    for strength, reach in repulsion:
        s = jnp.maximum(reach - r, 0.0)
        g3 = (s * s) * (s * (4.0 * strength))
        pslope = pslope + g3
        rep = g3 * s if rep is None else rep + g3 * s
    pval = pval - 0.25 * rep
    f = (pslope + (si + sj) * dslope) * rinv
    return f * dx, f * dy, f * dz, pval


def kernel(h_ref, u_ref, tab_ref, force_ref, energy_ref,
           dest_ref, tc_ref, tx_ref, rho_ref, sl_ref, em_ref, jd_ref, jf_ref, tf_ref):
    f32 = jnp.float32
    row = lax.broadcasted_iota(jnp.int32, (64, 256), 0)
    lane = lax.broadcasted_iota(jnp.int32, (64, 256), 1)
    xa = h_ref[0] + (row // 8 - 2).astype(f32) * SPAN_XY
    ya = h_ref[1] + (row % 8 - 2).astype(f32) * SPAN_XY
    za = h_ref[2] + (lane // 64 - 1).astype(f32) * SPAN_Z
    fb = jnp.floor((za + (ZOFF + 6 * HB)) * (1.0 / HB))
    valid = (fb >= 0.0) & (fb < float(NB))
    bins = jnp.where(valid, fb, -1.0)

    biota = lax.broadcasted_iota(jnp.int32, (32, 256), 0).astype(f32)
    upper = u_ref[...]
    ranks = []
    for c in range(64):
        ob = jnp.where(bins[c : c + 1, :] == biota, 1.0, 0.0)
        pr = jnp.dot(ob, upper, preferred_element_type=f32)
        ranks.append(jnp.sum(ob * pr, axis=0, keepdims=True))
    rank = jnp.concatenate(ranks, axis=0)
    over = valid & (rank >= float(CAP))
    overf = jnp.where(over, 1.0, 0.0)
    orank = jnp.dot(overf, upper, preferred_element_type=f32)
    novf = jnp.max(jnp.where(over, orank + 1.0, 0.0)).astype(jnp.int32)
    nch = (novf + 7) // 8
    dest = jnp.where(over, orank + float(MAIN), bins * float(CAP) + rank)
    dest_ref[...] = jnp.where(valid, dest, -1.0)

    tc_ref[...] = jnp.zeros_like(tc_ref)
    pos = [split3(v) for v in (xa, ya, za)]
    ones = jnp.where(valid, 1.0, 0.0)
    siota = lax.broadcasted_iota(jnp.int32, (256, 256), 0).astype(f32)
    sub8 = lax.broadcasted_iota(jnp.int32, (8, 256), 0)

    def scatter(half):
        for g in range(8):
            parts = [p[8 * g : 8 * g + 8] for trio in pos for p in trio] + [ones[8 * g : 8 * g + 8]]
            acc = None
            for u in range(8):
                lhs = jnp.concatenate([jnp.where(sub8 == u, p, 0.0) for p in parts], axis=0)
                drow = dest_ref[8 * g + u : 8 * g + u + 1, :] - float(256 * half)
                oh = jnp.where(siota == drow, 1.0, 0.0)
                out = lax.dot_general(lhs, oh, (((1,), (1,)), ((), ())), preferred_element_type=f32)
                acc = out if acc is None else acc + out
            have = acc[72:80] > 0.5
            for k in range(3):
                v = acc[24 * k : 24 * k + 8] + acc[24 * k + 8 : 24 * k + 16] + acc[24 * k + 16 : 24 * k + 24]
                tc_ref[k, 8 * g : 8 * g + 8, 256 * half : 256 * half + 256] = jnp.where(have, v, FAR)

    scatter(0)

    @pl.when(nch > 4)
    def _():
        scatter(1)

    for k in range(3):
        tx_ref[k, 0:256, :] = tc_ref[k, :, 0:256].T

    @pl.when(nch > 4)
    def _():
        for k in range(3):
            tx_ref[k, 256:512, :] = tc_ref[k, :, 256:512].T

    def take(values, idx):
        return jnp.take_along_axis(values, idx, axis=1, mode="promise_in_bounds")

    def expand_dens(m):
        m8 = pl.multiple_of(m * 8, 8)
        vals = [tx_ref[k, pl.ds(m8, 8), :] for k in range(3)]
        for w in range(21):
            idx = tab_ref[T_DENS + w]
            for k in range(3):
                jd_ref[k, w, pl.ds(m8, 8), :] = take(vals[k], idx)

    pl.loop(0, NB + nch)(expand_dens)

    sub = lax.broadcasted_iota(jnp.int32, (8, 128), 0)
    lane128 = lax.broadcasted_iota(jnp.int32, (8, 128), 1)
    diag = sub == lane128 % 8

    def spread(v):
        return jnp.broadcast_to(jnp.sum(jnp.where(diag, v, 0.0), axis=0, keepdims=True), (8, 128))

    def total(v):
        return jnp.broadcast_to(jnp.sum(v, axis=0, keepdims=True), (8, 128))

    rho_ref[...] = jnp.ones_like(rho_ref)

    def dens_i(t, ic):
        i8 = pl.multiple_of(ic * 8, 8)
        xi, yi, zi = [spread(jd_ref[k, (2 * t + 1) * 3 + 1, pl.ds(i8, 8), :]) for k in range(3)]
        return jnp.where(xi > 0.5 * FAR, -FAR, xi), yi, zi

    def dens_j(acc, it, t, jc, count):
        for m in range(count):
            j8 = pl.multiple_of((jc + m) * 8, 8)
            for dx in range(3):
                for dy in range(3):
                    w = (2 * t + dx) * 3 + dy
                    xj, yj, zj = [jd_ref[k, w, pl.ds(j8, 8), :] for k in range(3)]
                    acc = acc + rho_tile(*it, xj, yj, zj, dx == 1 and dy == 1)
        return acc

    def dens_store(acc, t, ic):
        i8 = pl.multiple_of(ic * 8, 8)
        got = take(total(acc), tab_ref[T_BACK + t])
        rho_ref[pl.ds(i8, 8), :] = jnp.where(tab_ref[T_MASK + t] > 0, got, rho_ref[pl.ds(i8, 8), :])

    zero = jnp.zeros((8, 128), f32)

    def dens_main(n):
        e, t = n // 3, n % 3
        ic = e + 3
        it = dens_i(t, ic)
        acc = dens_j(zero, it, t, e, 7)
        acc = dens_j(acc, it, t, NB, 1)
        acc = lax.fori_loop(1, nch, lambda q, a: dens_j(a, it, t, NB + q, 1), acc)
        dens_store(acc, t, ic)

    @pl.when(nch == 0)
    def _():
        for w in range(21):
            for k in range(3):
                jd_ref[k, w, MAIN : MAIN + 8, :] = jnp.full((8, 128), FAR, f32)

    pl.loop(0, 66)(dens_main)

    def dens_over(n):
        q, t = n // 3, n % 3
        ic = NB + q
        it = dens_i(t, ic)
        acc = lax.fori_loop(0, 4, lambda g, a: dens_j(a, it, t, 7 * g, 7), zero)
        acc = lax.fori_loop(0, nch, lambda p, a: dens_j(a, it, t, NB + p, 1), acc)
        dens_store(acc, t, ic)

    pl.loop(0, 3 * nch)(dens_over)

    def embed_rows(start, size):
        occ = tx_ref[0, pl.ds(start, size), :] < 0.5 * FAR
        val, slo = embedding(rho_ref[pl.ds(start, size), :])
        em_ref[pl.ds(start, size), :] = jnp.where(occ, val, 0.0)
        sl_ref[pl.ds(start, size), :] = jnp.where(occ, slo, 0.0)

    embed_rows(0, 256)

    @pl.when(nch > 4)
    def _():
        embed_rows(256, 256)

    def expand_forc(m):
        m8 = pl.multiple_of(m * 8, 8)
        vals = [tx_ref[k, pl.ds(m8, 8), :] for k in range(3)] + [sl_ref[pl.ds(m8, 8), :]]
        for w in range(9):
            idx = tab_ref[T_FORC + w]
            for k in range(4):
                jf_ref[k, w, pl.ds(m8, 8), :] = take(vals[k], idx)

    pl.loop(3, NB + nch)(expand_forc)

    @pl.when(nch == 0)
    def _():
        for w in range(9):
            for k in range(4):
                jf_ref[k, w, MAIN : MAIN + 8, :] = jnp.full((8, 128), FAR if k < 3 else 0.0, f32)

    def forc_i(ic):
        i8 = pl.multiple_of(ic * 8, 8)
        xi, yi, zi, si = [spread(jf_ref[k, 4, pl.ds(i8, 8), :]) for k in range(4)]
        return jnp.where(xi > 0.5 * FAR, -FAR, xi), yi, zi, si

    def forc_j(acc, it, jc, count):
        for m in range(count):
            j8 = pl.multiple_of((jc + m) * 8, 8)
            for w in range(9):
                vals = [jf_ref[k, w, pl.ds(j8, 8), :] for k in range(4)]
                out = force_tile(*it, *vals, w == 4)
                acc = tuple(a + o for a, o in zip(acc, out))
        return acc

    def forc_store(acc, it, ic):
        i8 = pl.multiple_of(ic * 8, 8)
        keep = it[0] > -0.5 * FAR
        fback = tab_ref[T_FBACK]
        em = spread(take(em_ref[pl.ds(i8, 8), :], tab_ref[T_FORC + 4]))
        res = [total(a) for a in acc]
        res[3] = em + 0.5 * res[3]
        for k in range(4):
            tf_ref[k, pl.ds(i8, 8), :] = take(jnp.where(keep, res[k], 0.0), fback)

    zeros4 = (zero, zero, zero, zero)
    tf_ref[...] = jnp.zeros_like(tf_ref)

    def forc_main(n):
        ic = n + 6
        it = forc_i(ic)
        acc = forc_j(zeros4, it, n + 3, 7)
        acc = forc_j(acc, it, NB, 1)
        acc = lax.fori_loop(1, nch, lambda q, a: forc_j(a, it, NB + q, 1), acc)
        forc_store(acc, it, ic)

    pl.loop(0, 16)(forc_main)

    def forc_over(q):
        ic = NB + q
        it = forc_i(ic)
        acc = lax.fori_loop(0, 25, lambda g, a: forc_j(a, it, 3 + g, 1), zeros4)
        acc = lax.fori_loop(0, nch, lambda p, a: forc_j(a, it, NB + p, 1), acc)
        forc_store(acc, it, ic)

    pl.loop(0, nch)(forc_over)

    row16 = lax.broadcasted_iota(jnp.int32, (16, 256), 0)
    oiota = lax.broadcasted_iota(jnp.int32, (256, 128), 0).astype(f32)

    def gather(half):
        trans = [tf_ref[k, 256 * half : 256 * half + 256, :].T[0:16] for k in range(4)]
        parts = [p for v in trans for p in split3(v)]
        acc = None
        for c in range(16):
            col = (c // 4 + 2) * 8 + c % 4 + 2
            lhs = jnp.concatenate([jnp.where(row16 == c, p, 0.0) for p in parts], axis=0)
            drow = dest_ref[col : col + 1, 64:192] - float(256 * half)
            oh = jnp.where(oiota == drow, 1.0, 0.0)
            out = jnp.dot(lhs, oh, preferred_element_type=f32)
            acc = out if acc is None else acc + out
        return [acc[48 * k : 48 * k + 16] + acc[48 * k + 16 : 48 * k + 32] + acc[48 * k + 32 : 48 * k + 48] for k in range(4)]

    res = gather(0)
    for k in range(3):
        force_ref[k] = res[k]
    energy_ref[...] = res[3]

    @pl.when(nch > 4)
    def _():
        more = gather(1)
        for k in range(3):
            force_ref[k] = force_ref[k] + more[k]
        energy_ref[...] = energy_ref[...] + more[3]


def local(halo):
    upper = jnp.asarray(np.triu(np.ones((256, 256), np.float32), 1))
    tabs = jnp.asarray(index_tables())
    vm = pl.BlockSpec(memory_space=pltpu.VMEM)
    f32 = jnp.float32
    return pl.pallas_call(
        kernel,
        out_shape=(jax.ShapeDtypeStruct((3, 16, 128), f32), jax.ShapeDtypeStruct((16, 128), f32)),
        in_specs=[vm, vm, vm],
        out_specs=(vm, vm),
        scratch_shapes=[
            pltpu.VMEM((64, 256), f32),
            pltpu.VMEM((3, 128, NSLOT), f32),
            pltpu.VMEM((3, NSLOT, 128), f32),
            pltpu.VMEM((NSLOT, 128), f32),
            pltpu.VMEM((NSLOT, 128), f32),
            pltpu.VMEM((NSLOT, 128), f32),
            pltpu.VMEM((3, 21, NSLOT, 128), f32),
            pltpu.VMEM((4, 9, NSLOT, 128), f32),
            pltpu.VMEM((4, NSLOT, 128), f32),
        ],
        compiler_params=pltpu.CompilerParams(vmem_limit_bytes=60 * 1024 * 1024),
    )(halo, upper, tabs)


def with_halo(value, sides):
    for axis, dim, width in sides:
        count, length = (lax.axis_size(axis), value.shape[dim])
        up = [(i, (i + 1) % count) for i in range(count)]
        down = [(j, i) for i, j in up]
        last = lax.slice_in_dim(value, length - width, length, axis=dim)
        first = lax.slice_in_dim(value, 0, width, axis=dim)
        before = lax.ppermute(last, axis, up)
        after = lax.ppermute(first, axis, down)
        value = jnp.concatenate([before, value, after], axis=dim)
    return value


def on_device(positions, counts):
    cx, cy, cz = counts.shape
    slot = lax.broadcasted_iota(jnp.int32, (cx, cy, cz, SLOTS), 3)
    occupied = (slot < counts[..., None]).reshape(1, cx, cy, cz * SLOTS)
    packed = jnp.where(occupied, positions, 1.0e6)
    halo = with_halo(packed, (("gz", 3, SLOTS), ("gx", 1, 2), ("gy", 2, 2)))
    forces, energy = local(halo.reshape(3, 64, 256))
    return forces.reshape(3, cx, cy, cz * SLOTS), energy.reshape(cx, cy, cz * SLOTS)


def solution(mesh):
    return jax.shard_map(
        on_device,
        mesh=mesh,
        in_specs=(P(None, "gx", "gy", "gz"), P("gx", "gy", "gz")),
        out_specs=(P(None, "gx", "gy", "gz"), P("gx", "gy", "gz")),
        check_vma=False,
    )
```

```python
import functools

import jax
import jax.numpy as jnp
import numpy as np
from jax import lax
from jax.experimental import pallas as pl
from jax.experimental.pallas import tpu as pltpu
from jax.sharding import PartitionSpec as P

SLOTS = 64
lattice_const = 3.615
SPAN_XY = 2.0 * lattice_const
SPAN_Z = 4.0 * lattice_const
cut_radius = 5.50679
cut_width = 0.50037
dens_scale = 3.80362
beta_one = 0.17394
radius_three = -2.19885
energy_one = 201.458
energy_two = 0.00659288
radius_one = 0.83591
radius_two = 4.46867
alpha_one = 2.97758
alpha_two = 1.54927
shift_delta = 0.0086225
repulsion = ((4.0, 2.24), (40.0, 1.8), (1150.0, 1.2))
embed_zero = -2.28235
embed_curve = 1.35535
lower_terms = (-1.27775, -0.86074, 1.78804, 2.97571)
upper_quartic = 0.4
upper_damping = 0.3
LOG2E = 1.4426950408889634

HB = 1.836
ZOFF = 0.228
NB = 28
CAP = 8
MAIN = NB * CAP
NSLOT = 512
NCHUNK = NSLOT // 8
FAR = 1000.0


def index_tables():
    lane = np.arange(128)
    sub = np.arange(8)[:, None]
    unit = lane // 8
    cols = [unit, 16 + unit, 32 + unit % 4]
    rows = []
    for ce in cols:
        for dx in (-1, 0, 1):
            for dy in (-1, 0, 1):
                rows.append((ce // 6 + 1 + dx) * 8 + ce % 6 + 1 + dy)
    for dx in (-1, 0, 1):
        for dy in (-1, 0, 1):
            rows.append((unit // 4 + 2 + dx) * 8 + unit % 4 + 2 + dy)
    rows = np.stack(rows + [rows[0]] * 4).astype(np.int32)
    back, mask = [], []
    x, y = lane // 8 - 1, lane % 8 - 1
    inside = (lane < 64) & (x >= 0) & (x < 6) & (y >= 0) & (y < 6)
    ce = np.where(inside, x * 6 + y, 0)
    for t, (lo, hi) in enumerate(((0, 16), (16, 32), (32, 36))):
        ok = inside & (ce >= lo) & (ce < hi)
        back.append(np.where(ok, (ce - lo) * 8, 0) + sub)
        mask.append(np.broadcast_to(ok.astype(np.int32), (8, 128)))
    fback = np.where(lane < 16, lane * 8, 0) + sub
    return rows, np.stack(back + mask + [fback]).astype(np.int32)


W_FORC, W_ALL = 27, 36
T_BACK, T_MASK, T_FBACK = 0, 3, 6
SIGMA = float(np.sqrt(beta_one * LOG2E))
TAPER_K = float((SIGMA * cut_width) ** 4)
LN2 = float(np.log(2.0))


def split3(v):
    hi = v.astype(jnp.bfloat16).astype(jnp.float32)
    rest = v - hi
    mid = rest.astype(jnp.bfloat16).astype(jnp.float32)
    return hi, mid, rest - mid


def embedding(density):
    e = density - 1.0
    e2 = e * e
    e3 = e2 * e
    l0, l1, l2, l3 = lower_terms
    low = embed_zero + e2 * (0.5 * embed_curve + e * (l0 + e * (l1 + e * (l2 + e * l3))))
    lows = e * (embed_curve + e * (3.0 * l0 + e * (4.0 * l1 + e * (5.0 * l2 + e * (6.0 * l3)))))
    num = embed_zero + e2 * (0.5 * embed_curve + e * (l0 + e * upper_quartic))
    nums = e * (embed_curve + e * (3.0 * l0 + e * (4.0 * upper_quartic)))
    below = e < 0.0
    den = jnp.where(below, 1.0, 1.0 + upper_damping * e3)
    inv = 1.0 / den
    up = num * inv
    ups = (nums * den - num * (3.0 * upper_damping) * e2) * inv * inv
    return jnp.where(below, low, up), jnp.where(below, lows, ups)


def geometry(xi, yi, zi, xj, yj, zj, mask_self):
    dx, dy, dz = xj - xi, yj - yi, zj - zi
    r2 = dx * dx + dy * dy + dz * dz
    if mask_self:
        r2 = jnp.where(r2 < 0.25 * SIGMA**2, 25.0, r2)
    rinv = lax.rsqrt(r2)
    return dx, dy, dz, rinv, r2 * rinv


def taper_parts(r):
    t = jnp.minimum(r - cut_radius * SIGMA, 0.0)
    t2 = t * t
    q = t2 * t2
    root = lax.rsqrt(q + TAPER_K)
    return t, t2, q, root * root


def gaussian(r):
    rs = r - radius_three * SIGMA
    return rs, jnp.exp2(float(np.log2(dens_scale)) - rs * rs)


def rho_tile(xi, yi, zi, xj, yj, zj, mask_self):
    _, _, _, _, r = geometry(xi, yi, zi, xj, yj, zj, mask_self)
    _, _, q, inv = taper_parts(r)
    _, g = gaussian(r)
    return g * (q * inv)


def force_tile(xi, yi, zi, si, xj, yj, zj, sj, mask_self, terms):
    dx, dy, dz, rinv, r = geometry(xi, yi, zi, xj, yj, zj, mask_self)
    t, t2, q, inv = taper_parts(r)
    taper = q * inv
    tslope = (t * t2) * (inv * inv)
    rs, g = gaussian(r)
    dslope = g * (rs * taper * (-2.0 * LN2 / (4.0 * TAPER_K)) + tslope)
    k1, k2 = alpha_one / SIGMA, alpha_two / SIGMA
    u1 = jnp.exp2(r * (-k1 * LOG2E) + alpha_one * LOG2E * radius_one)
    u2 = jnp.exp2(r * (-k2 * LOG2E) + alpha_two * LOG2E * radius_two)
    y1 = u1 * (u1 - 1.0)
    y2 = u2 * (u2 - 1.0)
    base = (y1 - u1) * energy_one + ((y2 - u2) * energy_two + shift_delta)
    bslope = y1 * (-2.0 * k1 * energy_one / (4.0 * TAPER_K)) + y2 * (-2.0 * k2 * energy_two / (4.0 * TAPER_K))
    pval = base * taper
    pslope = bslope * taper + base * tslope
    rep = None
    for strength, reach in repulsion[:terms]:
        s = jnp.maximum(reach * SIGMA - r, 0.0)
        g3 = (s * s) * (s * (strength / (SIGMA**4 * TAPER_K)))
        pslope = pslope + g3
        rep = g3 * s if rep is None else rep + g3 * s
    f = (pslope + (si + sj) * dslope) * rinv
    return f * dx, f * dy, f * dz, pval, rep


def kernel(h_ref, row_ref, tab_ref, force_ref, energy_ref,
           dest_ref, tc_ref, tx_ref, rm_ref, rho_ref, sl_ref, em_ref, jd_ref, jf_ref, tf_ref):
    f32 = jnp.float32
    row = lax.broadcasted_iota(jnp.int32, (64, 256), 0)
    lane = lax.broadcasted_iota(jnp.int32, (64, 256), 1)
    za = h_ref[2] + (lane // 64 - 1).astype(f32) * SPAN_Z
    pos = [
        split3((h_ref[0] + (row // 8 - 2).astype(f32) * SPAN_XY) * SIGMA),
        split3((h_ref[1] + (row % 8 - 2).astype(f32) * SPAN_XY) * SIGMA),
        split3(za * SIGMA),
    ]
    fb = jnp.floor((za + (ZOFF + 6 * HB)) * (1.0 / HB))
    valid = (fb >= 0.0) & (fb < float(NB))
    bins = jnp.where(valid, fb, -1.0)

    irow = lax.broadcasted_iota(jnp.int32, (256, 256), 0)
    ilane = lax.broadcasted_iota(jnp.int32, (256, 256), 1)
    upper = jnp.where(irow < ilane, 1.0, 0.0)
    fold = jnp.where(irow[0:8] == ilane[0:8] // 32, 1.0, 0.0)
    biota = lax.broadcasted_iota(jnp.int32, (32, 256), 0).astype(f32)
    ranks = []
    for g in range(8):
        ob = jnp.concatenate(
            [jnp.where(bins[8 * g + u : 8 * g + u + 1, :] == biota, 1.0, 0.0) for u in range(8)], axis=0
        )
        pr = ob * jnp.dot(ob, upper, preferred_element_type=f32)
        ranks.append(jnp.dot(fold, pr, preferred_element_type=f32))
    rank = jnp.concatenate(ranks, axis=0)
    over = valid & (rank >= float(CAP))
    orank = jnp.dot(jnp.where(over, 1.0, 0.0), upper, preferred_element_type=f32)
    novf = jnp.max(jnp.where(over, orank + 1.0, 0.0)).astype(jnp.int32)
    nch = (novf + 7) // 8
    dest = jnp.where(over, orank + float(MAIN), bins * float(CAP) + rank)
    dest_ref[...] = jnp.where(valid, dest, -1.0)

    tc_ref[:, 192:256, :] = jnp.zeros((3, 64, NSLOT), f32)
    ones = jnp.where(valid, 1.0, 0.0)
    siota = irow.astype(f32)
    sub8 = lax.broadcasted_iota(jnp.int32, (8, 256), 0)

    def scatter(half):
        for g in range(8):
            parts = [p[8 * g : 8 * g + 8] for trio in pos for p in trio] + [ones[8 * g : 8 * g + 8]]
            acc = None
            for u in range(8):
                lhs = jnp.concatenate([jnp.where(sub8 == u, p, 0.0) for p in parts], axis=0)
                drow = dest_ref[8 * g + u : 8 * g + u + 1, :] - float(256 * half)
                oh = jnp.where(siota == drow, 1.0, 0.0)
                out = lax.dot_general(lhs, oh, (((1,), (1,)), ((), ())), preferred_element_type=f32)
                acc = out if acc is None else acc + out
            have = acc[72:80] > 0.5
            for k in range(3):
                for p in range(3):
                    v = acc[24 * k + 8 * p : 24 * k + 8 * p + 8]
                    if p == 0:
                        v = jnp.where(have, v, FAR)
                    tc_ref[k, 64 * p + 8 * g : 64 * p + 8 * g + 8, 256 * half : 256 * half + 256] = v

    def transpose(half):
        for k in range(3):
            tx_ref[k, 256 * half : 256 * half + 256, :] = tc_ref[k, :, 256 * half : 256 * half + 256].T

    scatter(0)
    transpose(0)

    @pl.when(nch > 4)
    def _():
        scatter(1)
        transpose(1)

    def take(values, idx):
        return jnp.take_along_axis(values, idx, axis=1, mode="promise_in_bounds")

    source = jnp.where(irow[:, 0:128] < 192, irow[:, 0:128] % 64, -1)

    def spreader(w):
        m = jnp.where(source == row_ref[w : w + 1, :], 1.0, 0.0)
        rm_ref[w] = m
        return m

    def expand(values, first, count, out_ref, stride, comps):
        for w in range(0, count, 2):
            pair = [spreader(first + v) if comps[0] == 0 else rm_ref[first + v] for v in (w, w + 1) if v < count]
            mat = jnp.concatenate(pair, axis=1) if len(pair) == 2 else pair[0]
            for k, vals in zip(comps, values):
                out = jnp.dot(vals, mat, preferred_element_type=f32)
                for v in range(len(pair)):
                    for m in range(NB + 1):
                        out_ref[w + v, m * stride + k] = out[8 * m : 8 * m + 8, 128 * v : 128 * v + 128]

    def expand_more(values, first, count, out_ref, stride, comps, nch):
        def chunk(q):
            m8 = pl.multiple_of((NB + q) * 8, 8)

            def one(w):
                mat = rm_ref[first + w]
                for k, ref in zip(comps, values):
                    out_ref[w, (NB + q) * stride + k] = jnp.dot(ref[pl.ds(m8, 8), :], mat, preferred_element_type=f32)

            pl.loop(0, count)(one)

        pl.loop(1, nch)(chunk)

    rows = (NB + 1) * 8
    txk = [tx_ref.at[k] for k in range(3)]
    expand([tx_ref[k, 0:rows, :] for k in range(3)], 0, 27, jd_ref, 3, (0, 1, 2))
    expand([tx_ref[k, 0:rows, :] for k in range(3)], W_FORC, 9, jf_ref, 4, (0, 1, 2))
    expand_more(txk, 0, 27, jd_ref, 3, (0, 1, 2), nch)
    expand_more(txk, W_FORC, 9, jf_ref, 4, (0, 1, 2), nch)

    sub = lax.broadcasted_iota(jnp.int32, (8, 128), 0)
    lane128 = lax.broadcasted_iota(jnp.int32, (8, 128), 1)
    diag = sub == lane128 % 8

    def spread(v):
        return jnp.broadcast_to(jnp.sum(jnp.where(diag, v, 0.0), axis=0, keepdims=True), (8, 128))

    def total(v):
        return jnp.broadcast_to(jnp.sum(v, axis=0, keepdims=True), (8, 128))

    rho_ref[...] = jnp.ones_like(rho_ref)
    zero = jnp.zeros((8, 128), f32)

    def dens_i(t, ic):
        xi, yi, zi = [spread(jd_ref[9 * t + 4, ic * 3 + k]) for k in range(3)]
        return jnp.where(xi > 0.5 * FAR, -FAR, xi), yi, zi

    def dens_j(acc, it, t, jc, count):
        for m in range(count):
            for s in range(9):
                xj, yj, zj = [jd_ref[9 * t + s, (jc + m) * 3 + k] for k in range(3)]
                acc = acc + rho_tile(*it, xj, yj, zj, s == 4)
        return acc

    def dens_rest(acc, it, t):
        acc = dens_j(acc, it, t, NB, 1)
        return lax.fori_loop(1, nch, lambda q, a: dens_j(a, it, t, NB + q, 1), acc)

    def dens_store(acc, t, ic, group=0):
        i8 = pl.multiple_of(ic * 8, 8)
        got = take(acc, tab_ref[T_BACK + t] + 32 * group)
        rho_ref[pl.ds(i8, 8), :] = jnp.where(tab_ref[T_MASK + t] > 0, got, rho_ref[pl.ds(i8, 8), :])

    def dens_main(n):
        e, t = n // 2, n % 2
        it = dens_i(t, e + 3)
        acc = dens_rest(dens_j(zero, it, t, e, 7), it, t)
        dens_store(total(acc), t, e + 3)

    pl.loop(0, 44)(dens_main)

    def dens_corner(n):
        e = jnp.minimum(4 * n, 18)
        its = [dens_i(2, e + 3 + u) for u in range(4)]
        it = its[0]
        for u in range(1, 4):
            it = tuple(jnp.where(lane128 // 32 == u, b, a) for a, b in zip(it, its[u]))
        acc = total(dens_rest(dens_j(zero, it, 2, e, 10), it, 2))
        for u in range(4):
            dens_store(acc, 2, e + 3 + u, u)

    pl.loop(0, 6)(dens_corner)

    def dens_over(n):
        q, t = n // 3, n % 3
        ic = NB + q
        it = dens_i(t, ic)
        acc = lax.fori_loop(0, 4, lambda g, a: dens_j(a, it, t, 7 * g, 7), zero)
        acc = lax.fori_loop(0, nch, lambda p, a: dens_j(a, it, t, NB + p, 1), acc)
        dens_store(total(acc), t, ic)

    pl.loop(0, 3 * nch)(dens_over)

    low = lax.broadcasted_iota(jnp.int32, (256, 128), 1) < 64

    def embed_rows(start):
        occ = tx_ref[0, start : start + 256, 0:128] < 0.5 * FAR
        val, slo = embedding(rho_ref[start : start + 256, :])
        em_ref[start : start + 256, :] = jnp.where(occ, val, 0.0)
        hi, mid, lo = split3(jnp.where(occ & low, slo, 0.0))
        sl_ref[start : start + 256, 0:128] = hi + pltpu.roll(mid, 64, 1)
        sl_ref[start : start + 256, 128:256] = lo

    embed_rows(0)

    @pl.when(nch > 4)
    def _():
        embed_rows(256)

    expand([sl_ref[0:rows, :]], W_FORC, 9, jf_ref, 4, (3,))
    expand_more([sl_ref], W_FORC, 9, jf_ref, 4, (3,), nch)

    def forc_i(ic):
        xi, yi, zi, si = [spread(jf_ref[4, ic * 4 + k]) for k in range(4)]
        return jnp.where(xi > 0.5 * FAR, -FAR, xi), yi, zi, si

    def forc_j(acc, it, jc, terms):
        for m, n in enumerate(terms):
            for s in range(9):
                vals = [jf_ref[s, (jc + m) * 4 + k] for k in range(4)]
                out = force_tile(*it, *vals, s == 4, n)
                acc = tuple(a if o is None else a + o for a, o in zip(acc, out))
        return acc

    def forc_store(acc, it, ic):
        i8 = pl.multiple_of(ic * 8, 8)
        keep = it[0] > -0.5 * FAR
        idx = jnp.broadcast_to(row_ref[W_FORC + 4 : W_FORC + 5, :], (8, 128))
        em = spread(take(em_ref[pl.ds(i8, 8), :], idx))
        res = [total(a) * (SIGMA * 4.0 * TAPER_K) for a in acc[:3]]
        res.append(em + 0.5 * total(acc[3] - TAPER_K * acc[4]))
        for k in range(4):
            tf_ref[k, pl.ds(i8, 8), :] = take(jnp.where(keep, res[k], 0.0), tab_ref[T_FBACK])

    zeros5 = (zero,) * 5
    tf_ref[...] = jnp.zeros_like(tf_ref)

    def forc_main(n):
        ic = n + 6
        it = forc_i(ic)
        acc = forc_j(zeros5, it, n + 3, (0, 1, 3, 3, 3, 1, 0))
        acc = forc_j(acc, it, NB, (3,))
        acc = lax.fori_loop(1, nch, lambda q, a: forc_j(a, it, NB + q, (3,)), acc)
        forc_store(acc, it, ic)

    pl.loop(0, 16)(forc_main)

    def forc_over(q):
        ic = NB + q
        it = forc_i(ic)
        acc = lax.fori_loop(0, 5, lambda g, a: forc_j(a, it, 3 + 5 * g, (3,) * 5), zeros5)
        acc = lax.fori_loop(0, nch, lambda p, a: forc_j(a, it, NB + p, (3,)), acc)
        forc_store(acc, it, ic)

    pl.loop(0, nch)(forc_over)

    row16 = lax.broadcasted_iota(jnp.int32, (16, 256), 0)
    oiota = lax.broadcasted_iota(jnp.int32, (256, 128), 0).astype(f32)

    def gather(half):
        trans = [tf_ref[k, 256 * half : 256 * half + 256, :].T[0:16] for k in range(4)]
        parts = [p for v in trans for p in split3(v)]
        acc = None
        for c in range(16):
            col = (c // 4 + 2) * 8 + c % 4 + 2
            lhs = jnp.concatenate([jnp.where(row16 == c, p, 0.0) for p in parts], axis=0)
            drow = dest_ref[col : col + 1, 64:192] - float(256 * half)
            oh = jnp.where(oiota == drow, 1.0, 0.0)
            out = jnp.dot(lhs, oh, preferred_element_type=f32)
            acc = out if acc is None else acc + out
        return [acc[48 * k : 48 * k + 16] + acc[48 * k + 16 : 48 * k + 32] + acc[48 * k + 32 : 48 * k + 48] for k in range(4)]

    res = gather(0)
    for k in range(3):
        force_ref[k] = res[k]
    energy_ref[...] = res[3]

    @pl.when(nch > 4)
    def _():
        more = gather(1)
        for k in range(3):
            force_ref[k] = force_ref[k] + more[k]
        energy_ref[...] = energy_ref[...] + more[3]


def local(halo):
    rows, tabs = index_tables()
    vm = pl.BlockSpec(memory_space=pltpu.VMEM)
    f32 = jnp.float32
    return pl.pallas_call(
        kernel,
        out_shape=(jax.ShapeDtypeStruct((3, 16, 128), f32), jax.ShapeDtypeStruct((16, 128), f32)),
        in_specs=[vm, vm, vm],
        out_specs=(vm, vm),
        scratch_shapes=[
            pltpu.VMEM((64, 256), f32),
            pltpu.VMEM((3, 256, NSLOT), f32),
            pltpu.VMEM((3, NSLOT, 256), f32),
            pltpu.VMEM((W_ALL, 256, 128), f32),
            pltpu.VMEM((NSLOT, 128), f32),
            pltpu.VMEM((NSLOT, 256), f32),
            pltpu.VMEM((NSLOT, 128), f32),
            pltpu.VMEM((27, NCHUNK * 3, 8, 128), f32),
            pltpu.VMEM((9, NCHUNK * 4, 8, 128), f32),
            pltpu.VMEM((4, NSLOT, 128), f32),
        ],
        compiler_params=pltpu.CompilerParams(vmem_limit_bytes=60 * 1024 * 1024),
    )(halo, jnp.asarray(rows), jnp.asarray(tabs))


def with_halo(value, sides):
    for axis, dim, width in sides:
        count, length = (lax.axis_size(axis), value.shape[dim])
        up = [(i, (i + 1) % count) for i in range(count)]
        down = [(j, i) for i, j in up]
        last = lax.slice_in_dim(value, length - width, length, axis=dim)
        first = lax.slice_in_dim(value, 0, width, axis=dim)
        before = lax.ppermute(last, axis, up)
        after = lax.ppermute(first, axis, down)
        value = jnp.concatenate([before, value, after], axis=dim)
    return value


def on_device(positions, counts):
    cx, cy, cz = counts.shape
    slot = lax.broadcasted_iota(jnp.int32, (cx, cy, cz, SLOTS), 3)
    occupied = (slot < counts[..., None]).reshape(1, cx, cy, cz * SLOTS)
    packed = jnp.where(occupied, positions, 1.0e6)
    halo = with_halo(packed, (("gz", 3, SLOTS), ("gx", 1, 2), ("gy", 2, 2)))
    forces, energy = local(halo.reshape(3, 64, 256))
    return forces.reshape(3, cx, cy, cz * SLOTS), energy.reshape(cx, cy, cz * SLOTS)


def solution(mesh):
    return jax.shard_map(
        on_device,
        mesh=mesh,
        in_specs=(P(None, "gx", "gy", "gz"), P("gx", "gy", "gz")),
        out_specs=(P(None, "gx", "gy", "gz"), P("gx", "gy", "gz")),
        check_vma=False,
    )
```

```python
import functools

import jax
import jax.numpy as jnp
import numpy as np
from jax import lax
from jax.experimental import pallas as pl
from jax.experimental.pallas import tpu as pltpu
from jax.sharding import PartitionSpec as P

SLOTS = 64
lattice_const = 3.615
SPAN_XY = 2.0 * lattice_const
SPAN_Z = 4.0 * lattice_const
cut_radius = 5.50679
cut_width = 0.50037
dens_scale = 3.80362
beta_one = 0.17394
radius_three = -2.19885
energy_one = 201.458
energy_two = 0.00659288
radius_one = 0.83591
radius_two = 4.46867
alpha_one = 2.97758
alpha_two = 1.54927
shift_delta = 0.0086225
repulsion = ((4.0, 2.24), (40.0, 1.8), (1150.0, 1.2))
embed_zero = -2.28235
embed_curve = 1.35535
lower_terms = (-1.27775, -0.86074, 1.78804, 2.97571)
upper_quartic = 0.4
upper_damping = 0.3
LOG2E = 1.4426950408889634

HB = 1.836
ZOFF = 0.228
NB = 28
CAP = 8
MAIN = NB * CAP
NSLOT = 512
NCHUNK = NSLOT // 8
FAR = 1000.0


def index_tables():
    lane = np.arange(128)
    sub = np.arange(8)[:, None]
    unit = lane // 8
    cols = [unit, 16 + unit, 32 + unit % 4]
    rows = []
    for ce in cols:
        for dx in (-1, 0, 1):
            for dy in (-1, 0, 1):
                rows.append((ce // 6 + 1 + dx) * 8 + ce % 6 + 1 + dy)
    for dx in (-1, 0, 1):
        for dy in (-1, 0, 1):
            rows.append((unit // 4 + 2 + dx) * 8 + unit % 4 + 2 + dy)
    rows = np.stack(rows + [rows[0]] * 4).astype(np.int32)
    back, mask = [], []
    x, y = lane // 8 - 1, lane % 8 - 1
    inside = (lane < 64) & (x >= 0) & (x < 6) & (y >= 0) & (y < 6)
    ce = np.where(inside, x * 6 + y, 0)
    for t, (lo, hi) in enumerate(((0, 16), (16, 32), (32, 36))):
        ok = inside & (ce >= lo) & (ce < hi)
        back.append(np.where(ok, (ce - lo) * 8, 0) + sub)
        mask.append(np.broadcast_to(ok.astype(np.int32), (8, 128)))
    own = (lane < 64) & (lane // 8 >= 2) & (lane // 8 < 6) & (lane % 8 >= 2) & (lane % 8 < 6)
    fback = np.where(own, ((lane // 8 - 2) * 4 + lane % 8 - 2) * 8, 0) + sub
    return rows, np.stack(back + mask + [fback]).astype(np.int32)


W_FORC, W_ALL = 27, 36
T_BACK, T_MASK, T_FBACK = 0, 3, 6
SIGMA = float(np.sqrt(beta_one * LOG2E))
TAPER_K = float((SIGMA * cut_width) ** 4)
LN2 = float(np.log(2.0))


def split3(v):
    hi = v.astype(jnp.bfloat16).astype(jnp.float32)
    rest = v - hi
    mid = rest.astype(jnp.bfloat16).astype(jnp.float32)
    return hi, mid, rest - mid


def embedding(density):
    e = density - 1.0
    e2 = e * e
    e3 = e2 * e
    l0, l1, l2, l3 = lower_terms
    low = embed_zero + e2 * (0.5 * embed_curve + e * (l0 + e * (l1 + e * (l2 + e * l3))))
    lows = e * (embed_curve + e * (3.0 * l0 + e * (4.0 * l1 + e * (5.0 * l2 + e * (6.0 * l3)))))
    num = embed_zero + e2 * (0.5 * embed_curve + e * (l0 + e * upper_quartic))
    nums = e * (embed_curve + e * (3.0 * l0 + e * (4.0 * upper_quartic)))
    below = e < 0.0
    den = jnp.where(below, 1.0, 1.0 + upper_damping * e3)
    inv = 1.0 / den
    up = num * inv
    ups = (nums * den - num * (3.0 * upper_damping) * e2) * inv * inv
    return jnp.where(below, low, up), jnp.where(below, lows, ups)


def geometry(xi, yi, zi, xj, yj, zj, mask_self):
    dx, dy, dz = xj - xi, yj - yi, zj - zi
    r2 = dx * dx + dy * dy + dz * dz
    if mask_self:
        r2 = jnp.where(r2 < 0.25 * SIGMA**2, 25.0, r2)
    rinv = lax.rsqrt(r2)
    return dx, dy, dz, rinv, r2 * rinv


def taper_parts(r):
    t = jnp.minimum(r - cut_radius * SIGMA, 0.0)
    t2 = t * t
    q = t2 * t2
    root = lax.rsqrt(q + TAPER_K)
    return t, t2, q, root * root


def gaussian(r):
    rs = r - radius_three * SIGMA
    return rs, jnp.exp2(float(np.log2(dens_scale)) - rs * rs)


def rho_tile(xi, yi, zi, xj, yj, zj, mask_self):
    _, _, _, _, r = geometry(xi, yi, zi, xj, yj, zj, mask_self)
    _, _, q, inv = taper_parts(r)
    _, g = gaussian(r)
    return g * (q * inv)


def force_tile(xi, yi, zi, si, xj, yj, zj, sj, mask_self, terms):
    dx, dy, dz, rinv, r = geometry(xi, yi, zi, xj, yj, zj, mask_self)
    t, t2, q, inv = taper_parts(r)
    taper = q * inv
    tslope = (t * t2) * (inv * inv)
    rs, g = gaussian(r)
    dslope = g * (rs * taper * (-2.0 * LN2 / (4.0 * TAPER_K)) + tslope)
    k1, k2 = alpha_one / SIGMA, alpha_two / SIGMA
    u1 = jnp.exp2(r * (-k1 * LOG2E) + alpha_one * LOG2E * radius_one)
    u2 = jnp.exp2(r * (-k2 * LOG2E) + alpha_two * LOG2E * radius_two)
    y1 = u1 * (u1 - 1.0)
    y2 = u2 * (u2 - 1.0)
    base = (y1 - u1) * energy_one + ((y2 - u2) * energy_two + shift_delta)
    bslope = y1 * (-2.0 * k1 * energy_one / (4.0 * TAPER_K)) + y2 * (-2.0 * k2 * energy_two / (4.0 * TAPER_K))
    pval = base * taper
    pslope = bslope * taper + base * tslope
    rep = None
    for strength, reach in repulsion[:terms]:
        s = jnp.maximum(reach * SIGMA - r, 0.0)
        g3 = (s * s) * (s * (strength / (SIGMA**4 * TAPER_K)))
        pslope = pslope + g3
        rep = g3 * s if rep is None else rep + g3 * s
    f = (pslope + (si + sj) * dslope) * rinv
    return f * dx, f * dy, f * dz, pval, rep


def kernel(h_ref, row_ref, tab_ref, force_ref, energy_ref,
           dest_ref, tc_ref, tx_ref, rm_ref, rho_ref, sl_ref, em_ref, jd_ref, jf_ref, tf_ref,
           nat_ref, oh_ref, lb_ref, oa_ref, os_ref):
    f32 = jnp.float32
    row = lax.broadcasted_iota(jnp.int32, (64, 256), 0)
    lane = lax.broadcasted_iota(jnp.int32, (64, 256), 1)
    za = h_ref[2] + (lane // 64 - 1).astype(f32) * SPAN_Z
    pos = [
        split3((h_ref[0] + (row // 8 - 2).astype(f32) * SPAN_XY) * SIGMA),
        split3((h_ref[1] + (row % 8 - 2).astype(f32) * SPAN_XY) * SIGMA),
        split3(za * SIGMA),
    ]
    fb = jnp.floor((za + (ZOFF + 6 * HB)) * (1.0 / HB))
    valid = (fb >= 0.0) & (fb < float(NB))
    bins = jnp.where(valid, fb, -1.0)

    irow = lax.broadcasted_iota(jnp.int32, (256, 256), 0)
    ilane = lax.broadcasted_iota(jnp.int32, (256, 256), 1)
    upper = jnp.where(irow < ilane, 1.0, 0.0)
    fold = jnp.where(irow[0:8] == ilane[0:8] // 32, 1.0, 0.0)
    biota = lax.broadcasted_iota(jnp.int32, (32, 256), 0).astype(f32)
    ranks = []
    for g in range(8):
        ob = jnp.concatenate(
            [jnp.where(bins[8 * g + u : 8 * g + u + 1, :] == biota, 1.0, 0.0) for u in range(8)], axis=0
        )
        pr = ob * jnp.dot(ob, upper, preferred_element_type=f32)
        ranks.append(jnp.dot(fold, pr, preferred_element_type=f32))
    rank = jnp.concatenate(ranks, axis=0)
    over = valid & (rank >= float(CAP))
    orank = jnp.dot(jnp.where(over, 1.0, 0.0), upper, preferred_element_type=f32)
    novf = jnp.max(jnp.where(over, orank + 1.0, 0.0)).astype(jnp.int32)
    nch = (novf + 7) // 8
    count = jnp.sum(jnp.where(over, 1.0, 0.0)).astype(jnp.int32)
    slow = (nch > 1) | (count > 128)
    nslow = jnp.where(slow, nch, 0)
    quads = jnp.where(slow, 0, (count + 3) // 4)
    dest = jnp.where(over, orank + float(MAIN), bins * float(CAP) + rank)
    dest_ref[...] = jnp.where(valid, dest, -1.0)

    tc_ref[:, 192:256, :] = jnp.zeros((3, 64, NSLOT), f32)
    ones = jnp.where(valid, 1.0, 0.0)
    siota = irow.astype(f32)
    sub8 = lax.broadcasted_iota(jnp.int32, (8, 256), 0)

    def scatter(half):
        for g in range(8):
            parts = [p[8 * g : 8 * g + 8] for trio in pos for p in trio] + [ones[8 * g : 8 * g + 8]]
            acc = None
            for u in range(8):
                lhs = jnp.concatenate([jnp.where(sub8 == u, p, 0.0) for p in parts], axis=0)
                drow = dest_ref[8 * g + u : 8 * g + u + 1, :] - float(256 * half)
                oh = jnp.where(siota == drow, 1.0, 0.0)
                out = lax.dot_general(lhs, oh, (((1,), (1,)), ((), ())), preferred_element_type=f32)
                acc = out if acc is None else acc + out
            have = acc[72:80] > 0.5
            for k in range(3):
                for p in range(3):
                    v = acc[24 * k + 8 * p : 24 * k + 8 * p + 8]
                    if p == 0:
                        v = jnp.where(have, v, FAR)
                    tc_ref[k, 64 * p + 8 * g : 64 * p + 8 * g + 8, 256 * half : 256 * half + 256] = v

    def transpose(half):
        for k in range(3):
            tx_ref[k, 256 * half : 256 * half + 256, :] = tc_ref[k, :, 256 * half : 256 * half + 256].T

    scatter(0)
    transpose(0)

    @pl.when(nch > 4)
    def _():
        scatter(1)
        transpose(1)

    def take(values, idx):
        return jnp.take_along_axis(values, idx, axis=1, mode="promise_in_bounds")

    source = jnp.where(irow[:, 0:128] < 192, irow[:, 0:128] % 64, -1)

    def spreader(w):
        m = jnp.where(source == row_ref[w : w + 1, :], 1.0, 0.0)
        rm_ref[w] = m
        return m

    def expand(values, first, count, out_ref, stride, comps):
        for w in range(0, count, 2):
            pair = [spreader(first + v) if comps[0] == 0 else rm_ref[first + v] for v in (w, w + 1) if v < count]
            mat = jnp.concatenate(pair, axis=1) if len(pair) == 2 else pair[0]
            for k, vals in zip(comps, values):
                out = jnp.dot(vals, mat, preferred_element_type=f32)
                for v in range(len(pair)):
                    for m in range(NB + 1):
                        out_ref[w + v, m * stride + k] = out[8 * m : 8 * m + 8, 128 * v : 128 * v + 128]

    def expand_more(values, first, count, out_ref, stride, comps, nch):
        def chunk(q):
            m8 = pl.multiple_of((NB + q) * 8, 8)

            def one(w):
                mat = rm_ref[first + w]
                for k, ref in zip(comps, values):
                    out_ref[w, (NB + q) * stride + k] = jnp.dot(ref[pl.ds(m8, 8), :], mat, preferred_element_type=f32)

            pl.loop(0, count)(one)

        pl.loop(1, nch)(chunk)

    rows = (NB + 1) * 8
    txk = [tx_ref.at[k] for k in range(3)]
    expand([tx_ref[k, 0:rows, :] for k in range(3)], 0, 27, jd_ref, 3, (0, 1, 2))
    expand([tx_ref[k, 0:rows, :] for k in range(3)], W_FORC, 9, jf_ref, 4, (0, 1, 2))
    expand_more(txk, 0, 27, jd_ref, 3, (0, 1, 2), nch)
    expand_more(txk, W_FORC, 9, jf_ref, 4, (0, 1, 2), nch)

    sub = lax.broadcasted_iota(jnp.int32, (8, 128), 0)
    lane128 = lax.broadcasted_iota(jnp.int32, (8, 128), 1)
    diag = sub == lane128 % 8

    def spread(v):
        return jnp.broadcast_to(jnp.sum(jnp.where(diag, v, 0.0), axis=0, keepdims=True), (8, 128))

    def total(v):
        return jnp.broadcast_to(jnp.sum(v, axis=0, keepdims=True), (8, 128))

    rho_ref[...] = jnp.ones_like(rho_ref)
    zero = jnp.zeros((8, 128), f32)

    def dens_i(t, ic):
        xi, yi, zi = [spread(jd_ref[9 * t + 4, ic * 3 + k]) for k in range(3)]
        return jnp.where(xi > 0.5 * FAR, -FAR, xi), yi, zi

    def dens_j(acc, it, t, jc, count):
        for m in range(count):
            for s in range(9):
                xj, yj, zj = [jd_ref[9 * t + s, (jc + m) * 3 + k] for k in range(3)]
                acc = acc + rho_tile(*it, xj, yj, zj, s == 4)
        return acc

    def dens_rest(acc, it, t):
        return lax.fori_loop(0, nslow, lambda q, a: dens_j(a, it, t, NB + q, 1), acc)

    def dens_store(acc, t, ic, group=0):
        i8 = pl.multiple_of(ic * 8, 8)
        got = take(acc, tab_ref[T_BACK + t] + 32 * group)
        rho_ref[pl.ds(i8, 8), :] = jnp.where(tab_ref[T_MASK + t] > 0, got, rho_ref[pl.ds(i8, 8), :])

    def dens_main(n):
        e, t = n // 2, n % 2
        it = dens_i(t, e + 3)
        acc = dens_rest(dens_j(zero, it, t, e, 7), it, t)
        dens_store(total(acc), t, e + 3)

    pl.loop(0, 44)(dens_main)

    def dens_corner(n):
        e = jnp.minimum(4 * n, 18)
        its = [dens_i(2, e + 3 + u) for u in range(4)]
        it = its[0]
        for u in range(1, 4):
            it = tuple(jnp.where(lane128 // 32 == u, b, a) for a, b in zip(it, its[u]))
        acc = total(dens_rest(dens_j(zero, it, 2, e, 10), it, 2))
        for u in range(4):
            dens_store(acc, 2, e + 3 + u, u)

    pl.loop(0, 6)(dens_corner)

    def dens_over(n):
        q, t = n // 3, n % 3
        ic = NB + q
        it = dens_i(t, ic)
        acc = lax.fori_loop(0, 4, lambda g, a: dens_j(a, it, t, 7 * g, 7), zero)
        acc = lax.fori_loop(0, nslow, lambda p, a: dens_j(a, it, t, NB + p, 1), acc)
        dens_store(total(acc), t, ic)

    pl.loop(0, 3 * nslow)(dens_over)

    half = lane128 < 64
    mlow = lax.broadcasted_iota(jnp.int32, (rows, 128), 1) < 64
    for k in range(3):
        front = tx_ref[k, 0:rows, 0:128]
        full = front + pltpu.roll(front, 64, 1) + tx_ref[k, 0:rows, 128:256]
        full = jnp.where(mlow, full, 0.0)
        nat_ref[k, 0:rows, :] = full + pltpu.roll(full, 64, 1)
    present = half & (tx_ref[0, MAIN : MAIN + 8, 0:128] < 0.5 * FAR)
    lrow = lax.broadcasted_iota(jnp.int32, (128, 128), 0)

    def over_rows(front, back):
        return jnp.where(present, front + pltpu.roll(front, 64, 1) + back, 0.0)

    def to_list(values, empty):
        acc = jnp.zeros((128, 128), f32)
        for r in range(8):
            acc = acc + oh_ref[r] * values[r : r + 1, :]
        acc = jnp.broadcast_to(jnp.sum(acc, axis=1, keepdims=True), (128, 128))
        return jnp.where(lrow < count, acc, empty)

    def list_pair(k, n, h):
        i = 4 * n + 2 * h
        one = jnp.broadcast_to(lb_ref[k, pl.ds(i, 1), :], (8, 128))
        two = jnp.broadcast_to(lb_ref[k, pl.ds(i + 1, 1), :], (8, 128))
        return jnp.where(half, one, two)

    def keep_sums(k, value, n, h):
        t = total(value)
        i = 4 * n + 2 * h
        os_ref[k, pl.ds(i, 1), :] = jnp.where(half, t, 0.0)[0:1]
        os_ref[k, pl.ds(i + 1, 1), :] = jnp.where(half, 0.0, t)[0:1]

    def from_list(k):
        res = jnp.broadcast_to(jnp.sum(os_ref[k], axis=1, keepdims=True), (128, 128))
        res = jnp.where(lrow < count, res, 0.0)
        return jnp.concatenate([jnp.sum(oh_ref[r] * res, axis=0, keepdims=True) for r in range(8)], axis=0)

    @pl.when(quads > 0)
    def _():
        there = jnp.where(present, 1.0, 0.0)
        up = upper[0:128, 0:128]
        before = jnp.dot(there, up, preferred_element_type=f32)
        sums = jnp.dot(there, jnp.ones((128, 128), f32), preferred_element_type=f32)
        tri = jnp.where(irow[0:8, 0:8] > ilane[0:8, 0:8], 1.0, 0.0)
        place = jnp.where(present, before + jnp.dot(tri, sums, preferred_element_type=f32), -1.0)
        lrowf = lrow.astype(f32)
        for r in range(8):
            oh_ref[r] = jnp.where(lrowf == place[r : r + 1, :], 1.0, 0.0)
        for k in range(3):
            lb_ref[k] = to_list(jnp.where(present, nat_ref[k, MAIN : MAIN + 8, :], 0.0), -FAR)
        oa_ref[0] = jnp.zeros((rows, 128), f32)

        def quad(n):
            for h in range(2):
                it = [list_pair(k, n, h) for k in range(3)]
                own = zero
                for m in range(NB + 1):
                    vals = [nat_ref[k, 8 * m : 8 * m + 8, :] for k in range(3)]
                    out = rho_tile(*it, *vals, m == NB)
                    own = own + out
                    if m < NB:
                        oa_ref[0, 8 * m : 8 * m + 8, :] = oa_ref[0, 8 * m : 8 * m + 8, :] + out
                keep_sums(0, own, n, h)

        pl.loop(0, quads)(quad)
        both = oa_ref[0, 0:MAIN, :]
        rho_ref[0:MAIN, :] = rho_ref[0:MAIN, :] + both + pltpu.roll(both, 64, 1)
        rho_ref[MAIN : MAIN + 8, :] = from_list(0)


    low = lax.broadcasted_iota(jnp.int32, (256, 128), 1) < 64

    def embed_rows(start):
        occ = tx_ref[0, start : start + 256, 0:128] < 0.5 * FAR
        val, slo = embedding(rho_ref[start : start + 256, :])
        em_ref[start : start + 256, :] = jnp.where(occ, val, 0.0)
        hi, mid, lo = split3(jnp.where(occ & low, slo, 0.0))
        sl_ref[start : start + 256, 0:128] = hi + pltpu.roll(mid, 64, 1)
        sl_ref[start : start + 256, 128:256] = lo

    embed_rows(0)

    @pl.when(nch > 4)
    def _():
        embed_rows(256)

    sfront = sl_ref[0:rows, 0:128]
    sfull = jnp.where(mlow, sfront + pltpu.roll(sfront, 64, 1) + sl_ref[0:rows, 128:256], 0.0)
    nat_ref[3, 0:rows, :] = sfull + pltpu.roll(sfull, 64, 1)
    expand([sl_ref[0:rows, :]], W_FORC, 9, jf_ref, 4, (3,))
    expand_more([sl_ref], W_FORC, 9, jf_ref, 4, (3,), nch)

    def forc_i(ic):
        xi, yi, zi, si = [spread(jf_ref[4, ic * 4 + k]) for k in range(4)]
        return jnp.where(xi > 0.5 * FAR, -FAR, xi), yi, zi, si

    def forc_j(acc, it, jc, terms):
        for m, n in enumerate(terms):
            for s in range(9):
                vals = [jf_ref[s, (jc + m) * 4 + k] for k in range(4)]
                out = force_tile(*it, *vals, s == 4, n)
                acc = tuple(a if o is None else a + o for a, o in zip(acc, out))
        return acc

    def forc_store(acc, it, ic):
        i8 = pl.multiple_of(ic * 8, 8)
        keep = it[0] > -0.5 * FAR
        idx = jnp.broadcast_to(row_ref[W_FORC + 4 : W_FORC + 5, :], (8, 128))
        em = spread(take(em_ref[pl.ds(i8, 8), :], idx))
        res = [total(a) * (SIGMA * 4.0 * TAPER_K) for a in acc[:3]]
        res.append(em + 0.5 * total(acc[3] - TAPER_K * acc[4]))
        for k in range(4):
            tf_ref[k, pl.ds(i8, 8), :] = take(jnp.where(keep, res[k], 0.0), tab_ref[T_FBACK])

    zeros5 = (zero,) * 5
    tf_ref[...] = jnp.zeros_like(tf_ref)

    def forc_main(n):
        ic = n + 6
        it = forc_i(ic)
        acc = forc_j(zeros5, it, n + 3, (0, 1, 3, 3, 3, 1, 0))
        acc = lax.fori_loop(0, nslow, lambda q, a: forc_j(a, it, NB + q, (3,)), acc)
        forc_store(acc, it, ic)

    pl.loop(0, 16)(forc_main)

    def forc_over(q):
        ic = NB + q
        it = forc_i(ic)
        acc = lax.fori_loop(0, 5, lambda g, a: forc_j(a, it, 3 + 5 * g, (3,) * 5), zeros5)
        acc = lax.fori_loop(0, nslow, lambda p, a: forc_j(a, it, NB + p, (3,)), acc)
        forc_store(acc, it, ic)

    pl.loop(0, nslow)(forc_over)

    @pl.when(quads > 0)
    def _():
        lb_ref[3] = to_list(over_rows(sl_ref[MAIN : MAIN + 8, 0:128], sl_ref[MAIN : MAIN + 8, 128:256]), 0.0)
        for k in range(4):
            oa_ref[k] = jnp.zeros((rows, 128), f32)

        def quad(n):
            for h in range(2):
                it = [list_pair(k, n, h) for k in range(4)]
                own = [zero] * 4
                for m in list(range(3, 25)) + [NB]:
                    vals = [nat_ref[k, 8 * m : 8 * m + 8, :] for k in range(4)]
                    fx, fy, fz, pv, rp = force_tile(*it, *vals, m == NB, 3)
                    out = (fx, fy, fz, pv - TAPER_K * rp)
                    own = [a + b for a, b in zip(own, out)]
                    if m < NB:
                        for k in range(4):
                            old = oa_ref[k, 8 * m : 8 * m + 8, :]
                            oa_ref[k, 8 * m : 8 * m + 8, :] = old - out[k] if k < 3 else old + out[k]
                for k in range(4):
                    keep_sums(k, own[k], n, h)

        pl.loop(0, quads)(quad)
        for k in range(4):
            scale = SIGMA * 4.0 * TAPER_K if k < 3 else 0.5
            both = oa_ref[k, 0:MAIN, :]
            tf_ref[k, 0:MAIN, :] = tf_ref[k, 0:MAIN, :] + (both + pltpu.roll(both, 64, 1)) * scale
            mine = from_list(k) * scale
            if k == 3:
                mine = mine + em_ref[MAIN : MAIN + 8, :]
            tf_ref[k, MAIN : MAIN + 8, :] = jnp.where(present, mine, 0.0)

    row16 = lax.broadcasted_iota(jnp.int32, (16, 256), 0)
    oiota = lax.broadcasted_iota(jnp.int32, (256, 128), 0).astype(f32)

    def gather(half):
        trans = []
        for k in range(4):
            flip = tf_ref[k, 256 * half : 256 * half + 256, :].T
            trans.append(jnp.concatenate([flip[8 * x + 2 : 8 * x + 6] for x in range(2, 6)], axis=0))
        parts = [p for v in trans for p in split3(v)]
        acc = None
        for c in range(16):
            col = (c // 4 + 2) * 8 + c % 4 + 2
            lhs = jnp.concatenate([jnp.where(row16 == c, p, 0.0) for p in parts], axis=0)
            drow = dest_ref[col : col + 1, 64:192] - float(256 * half)
            oh = jnp.where(oiota == drow, 1.0, 0.0)
            out = jnp.dot(lhs, oh, preferred_element_type=f32)
            acc = out if acc is None else acc + out
        return [acc[48 * k : 48 * k + 16] + acc[48 * k + 16 : 48 * k + 32] + acc[48 * k + 32 : 48 * k + 48] for k in range(4)]

    res = gather(0)
    for k in range(3):
        force_ref[k] = res[k]
    energy_ref[...] = res[3]

    @pl.when(nch > 4)
    def _():
        more = gather(1)
        for k in range(3):
            force_ref[k] = force_ref[k] + more[k]
        energy_ref[...] = energy_ref[...] + more[3]


def local(halo):
    rows, tabs = index_tables()
    vm = pl.BlockSpec(memory_space=pltpu.VMEM)
    f32 = jnp.float32
    return pl.pallas_call(
        kernel,
        out_shape=(jax.ShapeDtypeStruct((3, 16, 128), f32), jax.ShapeDtypeStruct((16, 128), f32)),
        in_specs=[vm, vm, vm],
        out_specs=(vm, vm),
        scratch_shapes=[
            pltpu.VMEM((64, 256), f32),
            pltpu.VMEM((3, 256, NSLOT), f32),
            pltpu.VMEM((3, NSLOT, 256), f32),
            pltpu.VMEM((W_ALL, 256, 128), f32),
            pltpu.VMEM((NSLOT, 128), f32),
            pltpu.VMEM((NSLOT, 256), f32),
            pltpu.VMEM((NSLOT, 128), f32),
            pltpu.VMEM((27, NCHUNK * 3, 8, 128), f32),
            pltpu.VMEM((9, NCHUNK * 4, 8, 128), f32),
            pltpu.VMEM((4, NSLOT, 128), f32),
            pltpu.VMEM((4, MAIN + 8, 128), f32),
            pltpu.VMEM((8, 128, 128), f32),
            pltpu.VMEM((4, 128, 128), f32),
            pltpu.VMEM((4, MAIN + 8, 128), f32),
            pltpu.VMEM((4, 128, 128), f32),
        ],
        compiler_params=pltpu.CompilerParams(vmem_limit_bytes=60 * 1024 * 1024),
    )(halo, jnp.asarray(rows), jnp.asarray(tabs))


def with_halo(value, sides):
    for axis, dim, width in sides:
        count, length = (lax.axis_size(axis), value.shape[dim])
        up = [(i, (i + 1) % count) for i in range(count)]
        down = [(j, i) for i, j in up]
        last = lax.slice_in_dim(value, length - width, length, axis=dim)
        first = lax.slice_in_dim(value, 0, width, axis=dim)
        before = lax.ppermute(last, axis, up)
        after = lax.ppermute(first, axis, down)
        value = jnp.concatenate([before, value, after], axis=dim)
    return value


def on_device(positions, counts):
    cx, cy, cz = counts.shape
    slot = lax.broadcasted_iota(jnp.int32, (cx, cy, cz, SLOTS), 3)
    occupied = (slot < counts[..., None]).reshape(1, cx, cy, cz * SLOTS)
    packed = jnp.where(occupied, positions, 1.0e6)
    halo = with_halo(packed, (("gz", 3, SLOTS), ("gx", 1, 2), ("gy", 2, 2)))
    forces, energy = local(halo.reshape(3, 64, 256))
    return forces.reshape(3, cx, cy, cz * SLOTS), energy.reshape(cx, cy, cz * SLOTS)


def solution(mesh):
    return jax.shard_map(
        on_device,
        mesh=mesh,
        in_specs=(P(None, "gx", "gy", "gz"), P("gx", "gy", "gz")),
        out_specs=(P(None, "gx", "gy", "gz"), P("gx", "gy", "gz")),
        check_vma=False,
    )
```

```python
import functools

import jax
import jax.numpy as jnp
import numpy as np
from jax import lax
from jax.experimental import pallas as pl
from jax.experimental.pallas import tpu as pltpu
from jax.sharding import PartitionSpec as P

SLOTS = 64
lattice_const = 3.615
SPAN_XY = 2.0 * lattice_const
SPAN_Z = 4.0 * lattice_const
cut_radius = 5.50679
cut_width = 0.50037
dens_scale = 3.80362
beta_one = 0.17394
radius_three = -2.19885
energy_one = 201.458
energy_two = 0.00659288
radius_one = 0.83591
radius_two = 4.46867
alpha_one = 2.97758
alpha_two = 1.54927
shift_delta = 0.0086225
repulsion = ((4.0, 2.24), (40.0, 1.8), (1150.0, 1.2))
embed_zero = -2.28235
embed_curve = 1.35535
lower_terms = (-1.27775, -0.86074, 1.78804, 2.97571)
upper_quartic = 0.4
upper_damping = 0.3
LOG2E = 1.4426950408889634

HB = 1.836
ZOFF = 0.228
NB = 28
CAP = 8
MAIN = NB * CAP
NSLOT = 512
NCHUNK = NSLOT // 8
FAR = 1000.0


def index_tables():
    lane = np.arange(128)
    sub = np.arange(8)[:, None]
    unit = lane // 8
    cols = [unit, 16 + unit, 32 + unit % 4]
    rows = []
    for ce in cols:
        for dx in (-1, 0, 1):
            for dy in (-1, 0, 1):
                rows.append((ce // 6 + 1 + dx) * 8 + ce % 6 + 1 + dy)
    for dx in (-1, 0, 1):
        for dy in (-1, 0, 1):
            rows.append((unit // 4 + 2 + dx) * 8 + unit % 4 + 2 + dy)
    rows = np.stack(rows + [rows[0]] * 4).astype(np.int32)
    back, mask = [], []
    x, y = lane // 8 - 1, lane % 8 - 1
    inside = (lane < 64) & (x >= 0) & (x < 6) & (y >= 0) & (y < 6)
    ce = np.where(inside, x * 6 + y, 0)
    for t, (lo, hi) in enumerate(((0, 16), (16, 32), (32, 36))):
        ok = inside & (ce >= lo) & (ce < hi)
        back.append(np.where(ok, (ce - lo) * 8, 0) + sub)
        mask.append(np.broadcast_to(ok.astype(np.int32), (8, 128)))
    own = (lane < 64) & (lane // 8 >= 2) & (lane // 8 < 6) & (lane % 8 >= 2) & (lane % 8 < 6)
    fback = np.where(own, ((lane // 8 - 2) * 4 + lane % 8 - 2) * 8, 0) + sub
    return rows, np.stack(back + mask + [fback]).astype(np.int32)


W_FORC, W_ALL = 27, 36
T_BACK, T_MASK, T_FBACK = 0, 3, 6
SIGMA = float(np.sqrt(beta_one * LOG2E))
TAPER_K = float((SIGMA * cut_width) ** 4)
LN2 = float(np.log(2.0))


def split3(v):
    hi = v.astype(jnp.bfloat16).astype(jnp.float32)
    rest = v - hi
    mid = rest.astype(jnp.bfloat16).astype(jnp.float32)
    return hi, mid, rest - mid


def embedding(density):
    e = density - 1.0
    e2 = e * e
    e3 = e2 * e
    l0, l1, l2, l3 = lower_terms
    low = embed_zero + e2 * (0.5 * embed_curve + e * (l0 + e * (l1 + e * (l2 + e * l3))))
    lows = e * (embed_curve + e * (3.0 * l0 + e * (4.0 * l1 + e * (5.0 * l2 + e * (6.0 * l3)))))
    num = embed_zero + e2 * (0.5 * embed_curve + e * (l0 + e * upper_quartic))
    nums = e * (embed_curve + e * (3.0 * l0 + e * (4.0 * upper_quartic)))
    below = e < 0.0
    den = jnp.where(below, 1.0, 1.0 + upper_damping * e3)
    inv = 1.0 / den
    up = num * inv
    ups = (nums * den - num * (3.0 * upper_damping) * e2) * inv * inv
    return jnp.where(below, low, up), jnp.where(below, lows, ups)


def geometry(xi, yi, zi, xj, yj, zj, mask_self):
    dx, dy, dz = xj - xi, yj - yi, zj - zi
    r2 = dx * dx + dy * dy + dz * dz
    if mask_self:
        r2 = jnp.where(r2 < 0.25 * SIGMA**2, 25.0, r2)
    rinv = lax.rsqrt(r2)
    return dx, dy, dz, rinv, r2 * rinv


def taper_parts(r):
    t = jnp.minimum(r - cut_radius * SIGMA, 0.0)
    t2 = t * t
    q = t2 * t2
    root = lax.rsqrt(q + TAPER_K)
    return t, t2, q, root * root


def gaussian(r):
    rs = r - radius_three * SIGMA
    return rs, jnp.exp2(float(np.log2(dens_scale)) - rs * rs)


def rho_tile(xi, yi, zi, xj, yj, zj, mask_self):
    _, _, _, _, r = geometry(xi, yi, zi, xj, yj, zj, mask_self)
    _, _, q, inv = taper_parts(r)
    _, g = gaussian(r)
    return g * (q * inv)


def force_tile(xi, yi, zi, si, xj, yj, zj, sj, mask_self, terms):
    dx, dy, dz, rinv, r = geometry(xi, yi, zi, xj, yj, zj, mask_self)
    t, t2, q, inv = taper_parts(r)
    taper = q * inv
    tslope = (t * t2) * (inv * inv)
    rs, g = gaussian(r)
    dslope = g * (rs * taper * (-2.0 * LN2 / (4.0 * TAPER_K)) + tslope)
    k1, k2 = alpha_one / SIGMA, alpha_two / SIGMA
    u1 = jnp.exp2(r * (-k1 * LOG2E) + alpha_one * LOG2E * radius_one)
    u2 = jnp.exp2(r * (-k2 * LOG2E) + alpha_two * LOG2E * radius_two)
    y1 = u1 * (u1 - 1.0)
    y2 = u2 * (u2 - 1.0)
    base = (y1 - u1) * energy_one + ((y2 - u2) * energy_two + shift_delta)
    bslope = y1 * (-2.0 * k1 * energy_one / (4.0 * TAPER_K)) + y2 * (-2.0 * k2 * energy_two / (4.0 * TAPER_K))
    pval = base * taper
    pslope = bslope * taper + base * tslope
    rep = None
    for strength, reach in repulsion[:terms]:
        s = jnp.maximum(reach * SIGMA - r, 0.0)
        g3 = (s * s) * (s * (strength / (SIGMA**4 * TAPER_K)))
        pslope = pslope + g3
        rep = g3 * s if rep is None else rep + g3 * s
    f = (pslope + (si + sj) * dslope) * rinv
    return f * dx, f * dy, f * dz, pval, rep


def kernel(h_ref, row_ref, tab_ref, force_ref, energy_ref,
           dest_ref, tc_ref, tx_ref, rm_ref, rho_ref, sl_ref, em_ref, jd_ref, jf_ref, tf_ref,
           nat_ref, oh_ref, lb_ref, oa_ref, os_ref):
    f32 = jnp.float32
    row = lax.broadcasted_iota(jnp.int32, (64, 256), 0)
    lane = lax.broadcasted_iota(jnp.int32, (64, 256), 1)
    za = h_ref[2] + (lane // 64 - 1).astype(f32) * SPAN_Z
    pos = [
        split3((h_ref[0] + (row // 8 - 2).astype(f32) * SPAN_XY) * SIGMA),
        split3((h_ref[1] + (row % 8 - 2).astype(f32) * SPAN_XY) * SIGMA),
        split3(za * SIGMA),
    ]
    fb = jnp.floor((za + (ZOFF + 6 * HB)) * (1.0 / HB))
    valid = (fb >= 0.0) & (fb < float(NB))
    bins = jnp.where(valid, fb, -1.0)

    irow = lax.broadcasted_iota(jnp.int32, (256, 256), 0)
    ilane = lax.broadcasted_iota(jnp.int32, (256, 256), 1)
    upper = jnp.where(irow < ilane, 1.0, 0.0)
    fold = jnp.where(irow[0:8] == ilane[0:8] // 32, 1.0, 0.0)
    biota = lax.broadcasted_iota(jnp.int32, (32, 256), 0).astype(f32)
    ranks = []
    for g in range(8):
        ob = jnp.concatenate(
            [jnp.where(bins[8 * g + u : 8 * g + u + 1, :] == biota, 1.0, 0.0) for u in range(8)], axis=0
        )
        pr = ob * jnp.dot(ob, upper, preferred_element_type=f32)
        ranks.append(jnp.dot(fold, pr, preferred_element_type=f32))
    rank = jnp.concatenate(ranks, axis=0)
    over = valid & (rank >= float(CAP))
    orank = jnp.dot(jnp.where(over, 1.0, 0.0), upper, preferred_element_type=f32)
    novf = jnp.max(jnp.where(over, orank + 1.0, 0.0)).astype(jnp.int32)
    nch = (novf + 7) // 8
    count = jnp.sum(jnp.where(over, 1.0, 0.0)).astype(jnp.int32)
    slow = (nch > 1) | (count > 128)
    nslow = jnp.where(slow, nch, 0)
    quads = jnp.where(slow, 0, (count + 3) // 4)
    dest = jnp.where(over, orank + float(MAIN), bins * float(CAP) + rank)
    dest_ref[...] = jnp.where(valid, dest, -1.0)

    tc_ref[:, 192:256, :] = jnp.zeros((3, 64, NSLOT), f32)
    ones = jnp.where(valid, 1.0, 0.0)
    siota = irow.astype(f32)
    sub8 = lax.broadcasted_iota(jnp.int32, (8, 256), 0)

    def scatter(half):
        for g in range(8):
            parts = [p[8 * g : 8 * g + 8] for trio in pos for p in trio] + [ones[8 * g : 8 * g + 8]]
            acc = None
            for u in range(8):
                lhs = jnp.concatenate([jnp.where(sub8 == u, p, 0.0) for p in parts], axis=0)
                drow = dest_ref[8 * g + u : 8 * g + u + 1, :] - float(256 * half)
                oh = jnp.where(siota == drow, 1.0, 0.0)
                out = lax.dot_general(lhs, oh, (((1,), (1,)), ((), ())), preferred_element_type=f32)
                acc = out if acc is None else acc + out
            have = acc[72:80] > 0.5
            for k in range(3):
                for p in range(3):
                    v = acc[24 * k + 8 * p : 24 * k + 8 * p + 8]
                    if p == 0:
                        v = jnp.where(have, v, FAR)
                    tc_ref[k, 64 * p + 8 * g : 64 * p + 8 * g + 8, 256 * half : 256 * half + 256] = v

    def transpose(half):
        for k in range(3):
            tx_ref[k, 256 * half : 256 * half + 256, :] = tc_ref[k, :, 256 * half : 256 * half + 256].T

    scatter(0)
    transpose(0)

    @pl.when(nch > 4)
    def _():
        scatter(1)
        transpose(1)

    def take(values, idx):
        return jnp.take_along_axis(values, idx, axis=1, mode="promise_in_bounds")

    source = jnp.where(irow[:, 0:128] < 192, irow[:, 0:128] % 64, -1)

    def spreader(w):
        m = jnp.where(source == row_ref[w : w + 1, :], 1.0, 0.0)
        rm_ref[w] = m
        return m

    def expand(values, first, count, out_ref, stride, comps):
        for w in range(0, count, 2):
            pair = [spreader(first + v) if comps[0] == 0 else rm_ref[first + v] for v in (w, w + 1) if v < count]
            mat = jnp.concatenate(pair, axis=1) if len(pair) == 2 else pair[0]
            for k, vals in zip(comps, values):
                out = jnp.dot(vals, mat, preferred_element_type=f32)
                for v in range(len(pair)):
                    for m in range(NB + 1):
                        out_ref[w + v, m * stride + k] = out[8 * m : 8 * m + 8, 128 * v : 128 * v + 128]

    def expand_more(values, first, count, out_ref, stride, comps, nch):
        def chunk(q):
            m8 = pl.multiple_of((NB + q) * 8, 8)

            def one(w):
                mat = rm_ref[first + w]
                for k, ref in zip(comps, values):
                    out_ref[w, (NB + q) * stride + k] = jnp.dot(ref[pl.ds(m8, 8), :], mat, preferred_element_type=f32)

            pl.loop(0, count)(one)

        pl.loop(1, nch)(chunk)

    rows = (NB + 1) * 8
    txk = [tx_ref.at[k] for k in range(3)]
    expand([tx_ref[k, 0:rows, :] for k in range(3)], 0, 27, jd_ref, 3, (0, 1, 2))
    expand([tx_ref[k, 0:rows, :] for k in range(3)], W_FORC, 9, jf_ref, 4, (0, 1, 2))
    expand_more(txk, 0, 27, jd_ref, 3, (0, 1, 2), nch)
    expand_more(txk, W_FORC, 9, jf_ref, 4, (0, 1, 2), nch)

    sub = lax.broadcasted_iota(jnp.int32, (8, 128), 0)
    lane128 = lax.broadcasted_iota(jnp.int32, (8, 128), 1)
    diag = sub == lane128 % 8

    def spread(v):
        return jnp.broadcast_to(jnp.sum(jnp.where(diag, v, 0.0), axis=0, keepdims=True), (8, 128))

    def total(v):
        return jnp.broadcast_to(jnp.sum(v, axis=0, keepdims=True), (8, 128))

    rho_ref[...] = jnp.ones_like(rho_ref)
    zero = jnp.zeros((8, 128), f32)

    def dens_i(t, ic):
        xi, yi, zi = [spread(jd_ref[9 * t + 4, ic * 3 + k]) for k in range(3)]
        return jnp.where(xi > 0.5 * FAR, -FAR, xi), yi, zi

    def dens_j(acc, it, t, jc, count):
        for m in range(count):
            for s in range(9):
                xj, yj, zj = [jd_ref[9 * t + s, (jc + m) * 3 + k] for k in range(3)]
                acc = acc + rho_tile(*it, xj, yj, zj, s == 4)
        return acc

    def dens_rest(acc, it, t):
        return lax.fori_loop(0, nslow, lambda q, a: dens_j(a, it, t, NB + q, 1), acc)

    def dens_store(acc, t, ic, group=0):
        i8 = pl.multiple_of(ic * 8, 8)
        got = take(acc, tab_ref[T_BACK + t] + 32 * group)
        rho_ref[pl.ds(i8, 8), :] = jnp.where(tab_ref[T_MASK + t] > 0, got, rho_ref[pl.ds(i8, 8), :])

    def dens_main(n):
        e, t = 2 * (n // 2), n % 2
        its = [dens_i(t, e + 3 + v) for v in range(2)]
        accs = [zero, zero]
        for m in range(8):
            for s in range(9):
                vals = [jd_ref[9 * t + s, (e + m) * 3 + k] for k in range(3)]
                for v in range(2):
                    if 0 <= m - v < 7:
                        accs[v] = accs[v] + rho_tile(*its[v], *vals, s == 4)
        for v in range(2):
            dens_store(total(dens_rest(accs[v], its[v], t)), t, e + 3 + v)

    pl.loop(0, 22)(dens_main)

    def dens_corner(n):
        e = jnp.minimum(4 * n, 18)
        its = [dens_i(2, e + 3 + u) for u in range(4)]
        it = its[0]
        for u in range(1, 4):
            it = tuple(jnp.where(lane128 // 32 == u, b, a) for a, b in zip(it, its[u]))
        acc = total(dens_rest(dens_j(zero, it, 2, e, 10), it, 2))
        for u in range(4):
            dens_store(acc, 2, e + 3 + u, u)

    pl.loop(0, 6)(dens_corner)

    def dens_over(n):
        q, t = n // 3, n % 3
        ic = NB + q
        it = dens_i(t, ic)
        acc = lax.fori_loop(0, 4, lambda g, a: dens_j(a, it, t, 7 * g, 7), zero)
        acc = lax.fori_loop(0, nslow, lambda p, a: dens_j(a, it, t, NB + p, 1), acc)
        dens_store(total(acc), t, ic)

    pl.loop(0, 3 * nslow)(dens_over)

    half = lane128 < 64
    mlow = lax.broadcasted_iota(jnp.int32, (rows, 128), 1) < 64
    for k in range(3):
        front = tx_ref[k, 0:rows, 0:128]
        full = front + pltpu.roll(front, 64, 1) + tx_ref[k, 0:rows, 128:256]
        full = jnp.where(mlow, full, 0.0)
        nat_ref[k, 0:rows, :] = full + pltpu.roll(full, 64, 1)
    present = half & (tx_ref[0, MAIN : MAIN + 8, 0:128] < 0.5 * FAR)
    lrow = lax.broadcasted_iota(jnp.int32, (128, 128), 0)

    def over_rows(front, back):
        return jnp.where(present, front + pltpu.roll(front, 64, 1) + back, 0.0)

    def to_list(values, empty):
        acc = jnp.zeros((128, 128), f32)
        for r in range(8):
            acc = acc + oh_ref[r] * values[r : r + 1, :]
        acc = jnp.broadcast_to(jnp.sum(acc, axis=1, keepdims=True), (128, 128))
        return jnp.where(lrow < count, acc, empty)

    def list_pair(k, n, h):
        i = 4 * n + 2 * h
        one = jnp.broadcast_to(lb_ref[k, pl.ds(i, 1), :], (8, 128))
        two = jnp.broadcast_to(lb_ref[k, pl.ds(i + 1, 1), :], (8, 128))
        return jnp.where(half, one, two)

    def keep_sums(k, value, n, h):
        t = total(value)
        i = 4 * n + 2 * h
        os_ref[k, pl.ds(i, 1), :] = jnp.where(half, t, 0.0)[0:1]
        os_ref[k, pl.ds(i + 1, 1), :] = jnp.where(half, 0.0, t)[0:1]

    def from_list(k):
        res = jnp.broadcast_to(jnp.sum(os_ref[k], axis=1, keepdims=True), (128, 128))
        res = jnp.where(lrow < count, res, 0.0)
        return jnp.concatenate([jnp.sum(oh_ref[r] * res, axis=0, keepdims=True) for r in range(8)], axis=0)

    @pl.when(quads > 0)
    def _():
        there = jnp.where(present, 1.0, 0.0)
        up = upper[0:128, 0:128]
        before = jnp.dot(there, up, preferred_element_type=f32)
        sums = jnp.dot(there, jnp.ones((128, 128), f32), preferred_element_type=f32)
        tri = jnp.where(irow[0:8, 0:8] > ilane[0:8, 0:8], 1.0, 0.0)
        place = jnp.where(present, before + jnp.dot(tri, sums, preferred_element_type=f32), -1.0)
        lrowf = lrow.astype(f32)
        for r in range(8):
            oh_ref[r] = jnp.where(lrowf == place[r : r + 1, :], 1.0, 0.0)
        for k in range(3):
            lb_ref[k] = to_list(jnp.where(present, nat_ref[k, MAIN : MAIN + 8, :], 0.0), -FAR)
        oa_ref[0] = jnp.zeros((rows, 128), f32)

        def quad(n):
            for h in range(2):
                it = [list_pair(k, n, h) for k in range(3)]
                own = zero
                for m in range(NB + 1):
                    vals = [nat_ref[k, 8 * m : 8 * m + 8, :] for k in range(3)]
                    out = rho_tile(*it, *vals, m == NB)
                    own = own + out
                    if m < NB:
                        oa_ref[0, 8 * m : 8 * m + 8, :] = oa_ref[0, 8 * m : 8 * m + 8, :] + out
                keep_sums(0, own, n, h)

        pl.loop(0, quads)(quad)
        both = oa_ref[0, 0:MAIN, :]
        rho_ref[0:MAIN, :] = rho_ref[0:MAIN, :] + both + pltpu.roll(both, 64, 1)
        rho_ref[MAIN : MAIN + 8, :] = from_list(0)


    low = lax.broadcasted_iota(jnp.int32, (256, 128), 1) < 64

    def embed_rows(start):
        occ = tx_ref[0, start : start + 256, 0:128] < 0.5 * FAR
        val, slo = embedding(rho_ref[start : start + 256, :])
        em_ref[start : start + 256, :] = jnp.where(occ, val, 0.0)
        hi, mid, lo = split3(jnp.where(occ & low, slo, 0.0))
        sl_ref[start : start + 256, 0:128] = hi + pltpu.roll(mid, 64, 1)
        sl_ref[start : start + 256, 128:256] = lo

    embed_rows(0)

    @pl.when(nch > 4)
    def _():
        embed_rows(256)

    sfront = sl_ref[0:rows, 0:128]
    sfull = jnp.where(mlow, sfront + pltpu.roll(sfront, 64, 1) + sl_ref[0:rows, 128:256], 0.0)
    nat_ref[3, 0:rows, :] = sfull + pltpu.roll(sfull, 64, 1)
    expand([sl_ref[0:rows, :]], W_FORC, 9, jf_ref, 4, (3,))
    expand_more([sl_ref], W_FORC, 9, jf_ref, 4, (3,), nch)

    def forc_i(ic):
        xi, yi, zi, si = [spread(jf_ref[4, ic * 4 + k]) for k in range(4)]
        return jnp.where(xi > 0.5 * FAR, -FAR, xi), yi, zi, si

    def forc_j(acc, it, jc, terms):
        for m, n in enumerate(terms):
            for s in range(9):
                vals = [jf_ref[s, (jc + m) * 4 + k] for k in range(4)]
                out = force_tile(*it, *vals, s == 4, n)
                acc = tuple(a if o is None else a + o for a, o in zip(acc, out))
        return acc

    def forc_store(acc, it, ic):
        i8 = pl.multiple_of(ic * 8, 8)
        keep = it[0] > -0.5 * FAR
        idx = jnp.broadcast_to(row_ref[W_FORC + 4 : W_FORC + 5, :], (8, 128))
        em = spread(take(em_ref[pl.ds(i8, 8), :], idx))
        res = [total(a) * (SIGMA * 4.0 * TAPER_K) for a in acc[:3]]
        res.append(em + 0.5 * total(acc[3] - TAPER_K * acc[4]))
        for k in range(4):
            tf_ref[k, pl.ds(i8, 8), :] = take(jnp.where(keep, res[k], 0.0), tab_ref[T_FBACK])

    zeros5 = (zero,) * 5
    tf_ref[...] = jnp.zeros_like(tf_ref)

    def forc_main(n):
        ic = n + 6
        it = forc_i(ic)
        acc = forc_j(zeros5, it, n + 3, (0, 1, 3, 3, 3, 1, 0))
        acc = lax.fori_loop(0, nslow, lambda q, a: forc_j(a, it, NB + q, (3,)), acc)
        forc_store(acc, it, ic)

    pl.loop(0, 16)(forc_main)

    def forc_over(q):
        ic = NB + q
        it = forc_i(ic)
        acc = lax.fori_loop(0, 5, lambda g, a: forc_j(a, it, 3 + 5 * g, (3,) * 5), zeros5)
        acc = lax.fori_loop(0, nslow, lambda p, a: forc_j(a, it, NB + p, (3,)), acc)
        forc_store(acc, it, ic)

    pl.loop(0, nslow)(forc_over)

    @pl.when(quads > 0)
    def _():
        lb_ref[3] = to_list(over_rows(sl_ref[MAIN : MAIN + 8, 0:128], sl_ref[MAIN : MAIN + 8, 128:256]), 0.0)
        for k in range(4):
            oa_ref[k] = jnp.zeros((rows, 128), f32)

        def quad(n):
            for h in range(2):
                it = [list_pair(k, n, h) for k in range(4)]
                own = [zero] * 4
                for m in list(range(3, 25)) + [NB]:
                    vals = [nat_ref[k, 8 * m : 8 * m + 8, :] for k in range(4)]
                    fx, fy, fz, pv, rp = force_tile(*it, *vals, m == NB, 3)
                    out = (fx, fy, fz, pv - TAPER_K * rp)
                    own = [a + b for a, b in zip(own, out)]
                    if m < NB:
                        for k in range(4):
                            old = oa_ref[k, 8 * m : 8 * m + 8, :]
                            oa_ref[k, 8 * m : 8 * m + 8, :] = old - out[k] if k < 3 else old + out[k]
                for k in range(4):
                    keep_sums(k, own[k], n, h)

        pl.loop(0, quads)(quad)
        for k in range(4):
            scale = SIGMA * 4.0 * TAPER_K if k < 3 else 0.5
            both = oa_ref[k, 0:MAIN, :]
            tf_ref[k, 0:MAIN, :] = tf_ref[k, 0:MAIN, :] + (both + pltpu.roll(both, 64, 1)) * scale
            mine = from_list(k) * scale
            if k == 3:
                mine = mine + em_ref[MAIN : MAIN + 8, :]
            tf_ref[k, MAIN : MAIN + 8, :] = jnp.where(present, mine, 0.0)

    row16 = lax.broadcasted_iota(jnp.int32, (16, 256), 0)
    oiota = lax.broadcasted_iota(jnp.int32, (256, 128), 0).astype(f32)

    def gather(half):
        trans = []
        for k in range(4):
            flip = tf_ref[k, 256 * half : 256 * half + 256, :].T
            trans.append(jnp.concatenate([flip[8 * x + 2 : 8 * x + 6] for x in range(2, 6)], axis=0))
        parts = [p for v in trans for p in split3(v)]
        acc = None
        for c in range(16):
            col = (c // 4 + 2) * 8 + c % 4 + 2
            lhs = jnp.concatenate([jnp.where(row16 == c, p, 0.0) for p in parts], axis=0)
            drow = dest_ref[col : col + 1, 64:192] - float(256 * half)
            oh = jnp.where(oiota == drow, 1.0, 0.0)
            out = jnp.dot(lhs, oh, preferred_element_type=f32)
            acc = out if acc is None else acc + out
        return [acc[48 * k : 48 * k + 16] + acc[48 * k + 16 : 48 * k + 32] + acc[48 * k + 32 : 48 * k + 48] for k in range(4)]

    res = gather(0)
    for k in range(3):
        force_ref[k] = res[k]
    energy_ref[...] = res[3]

    @pl.when(nch > 4)
    def _():
        more = gather(1)
        for k in range(3):
            force_ref[k] = force_ref[k] + more[k]
        energy_ref[...] = energy_ref[...] + more[3]


def local(halo):
    rows, tabs = index_tables()
    vm = pl.BlockSpec(memory_space=pltpu.VMEM)
    f32 = jnp.float32
    return pl.pallas_call(
        kernel,
        out_shape=(jax.ShapeDtypeStruct((3, 16, 128), f32), jax.ShapeDtypeStruct((16, 128), f32)),
        in_specs=[vm, vm, vm],
        out_specs=(vm, vm),
        scratch_shapes=[
            pltpu.VMEM((64, 256), f32),
            pltpu.VMEM((3, 256, NSLOT), f32),
            pltpu.VMEM((3, NSLOT, 256), f32),
            pltpu.VMEM((W_ALL, 256, 128), f32),
            pltpu.VMEM((NSLOT, 128), f32),
            pltpu.VMEM((NSLOT, 256), f32),
            pltpu.VMEM((NSLOT, 128), f32),
            pltpu.VMEM((27, NCHUNK * 3, 8, 128), f32),
            pltpu.VMEM((9, NCHUNK * 4, 8, 128), f32),
            pltpu.VMEM((4, NSLOT, 128), f32),
            pltpu.VMEM((4, MAIN + 8, 128), f32),
            pltpu.VMEM((8, 128, 128), f32),
            pltpu.VMEM((4, 128, 128), f32),
            pltpu.VMEM((4, MAIN + 8, 128), f32),
            pltpu.VMEM((4, 128, 128), f32),
        ],
        compiler_params=pltpu.CompilerParams(vmem_limit_bytes=60 * 1024 * 1024),
    )(halo, jnp.asarray(rows), jnp.asarray(tabs))


def with_halo(value, sides):
    for axis, dim, width in sides:
        count, length = (lax.axis_size(axis), value.shape[dim])
        up = [(i, (i + 1) % count) for i in range(count)]
        down = [(j, i) for i, j in up]
        last = lax.slice_in_dim(value, length - width, length, axis=dim)
        first = lax.slice_in_dim(value, 0, width, axis=dim)
        before = lax.ppermute(last, axis, up)
        after = lax.ppermute(first, axis, down)
        value = jnp.concatenate([before, value, after], axis=dim)
    return value


def on_device(positions, counts):
    cx, cy, cz = counts.shape
    slot = lax.broadcasted_iota(jnp.int32, (cx, cy, cz, SLOTS), 3)
    occupied = (slot < counts[..., None]).reshape(1, cx, cy, cz * SLOTS)
    packed = jnp.where(occupied, positions, 1.0e6)
    halo = with_halo(packed, (("gz", 3, SLOTS), ("gx", 1, 2)))
    here, count = lax.axis_index("gy"), lax.axis_size("gy")
    peer = lax.broadcasted_iota(jnp.int32, (count, 1, 1, 1, 1), 0)
    send = jnp.where((peer - here + count) % count == 1, halo[None, :, :, cy - 2 :], halo[None, :, :, :2])
    got = lax.all_to_all(send, "gy", 0, 0)
    before = lax.dynamic_index_in_dim(got, (here + count - 1) % count, 0, keepdims=False)
    after = lax.dynamic_index_in_dim(got, (here + 1) % count, 0, keepdims=False)
    halo = jnp.concatenate([before, halo, after], axis=2)
    forces, energy = local(halo.reshape(3, 64, 256))
    return forces.reshape(3, cx, cy, cz * SLOTS), energy.reshape(cx, cy, cz * SLOTS)


def solution(mesh):
    return jax.shard_map(
        on_device,
        mesh=mesh,
        in_specs=(P(None, "gx", "gy", "gz"), P("gx", "gy", "gz")),
        out_specs=(P(None, "gx", "gy", "gz"), P("gx", "gy", "gz")),
        check_vma=False,
    )
```
